32 devices in a mesh: rep: 1, dp: 32 (over x, y, z, core).
Axes of the slice: x: 2, y: 2, z: 4, core: 2. Of those that a mesh axis runs over, the one named last changes fastest.
Arguments:
- x: bfloat16 [32, 2048, 1024], P(('rep', 'dp'))
- dy: bfloat16 [32, 2048, 1024], P(('rep', 'dp'))
- w_gate: bfloat16 [2, 1024, 2816], P(None, 'dp')
- w_up: bfloat16 [2, 1024, 2816], P(None, 'dp')
- w_down: bfloat16 [2, 2816, 1024], P(None, 'dp')
- m_w_gate: float32 [2, 1024, 2816], P(None, 'dp')
- m_w_up: float32 [2, 1024, 2816], P(None, 'dp')
- m_w_down: float32 [2, 2816, 1024], P(None, 'dp')
- v_w_gate: float32 [2, 1024, 2816], P(None, 'dp')
- v_w_up: float32 [2, 1024, 2816], P(None, 'dp')
- v_w_down: float32 [2, 2816, 1024], P(None, 'dp')
Outputs:
- output 1: bfloat16 [2, 1024, 2816], P('rep', 'dp')
- output 2: bfloat16 [2, 1024, 2816], P('rep', 'dp')
- output 3: bfloat16 [2, 2816, 1024], P('rep', 'dp')
- output 4: float32 [2, 1024, 2816], P('rep', 'dp')
- output 5: float32 [2, 1024, 2816], P('rep', 'dp')
- output 6: float32 [2, 2816, 1024], P('rep', 'dp')
- output 7: float32 [2, 1024, 2816], P('rep', 'dp')
- output 8: float32 [2, 1024, 2816], P('rep', 'dp')
- output 9: float32 [2, 2816, 1024], P('rep', 'dp')
All inputs are finite; a program needn't handle non-finite values.
Results may differ from the reference program's by a relative error of at most 0.0279.
Values are sent between devices in bfloat16 or wider.
A program may use at most 2 GiB of HBM per device.

```python
import jax
import jax.numpy as jnp
from jax import lax

SEQUENCES = 32
TOKENS = 2048
D = 1024
FF = 2816
LAYERS = 2
NAMES = ("w_gate", "w_up", "w_down")
SHAPES = {"w_gate": (LAYERS, D, FF), "w_up": (LAYERS, D, FF), "w_down": (LAYERS, FF, D)}


def bump(key, n, height):
    away = (jnp.arange(n, dtype=jnp.int32) - jax.random.randint(key, (), 0, n, jnp.int32)) % n
    return jnp.where(away < n // 8, height, 1.0)


def together(key, own, strength):
    shared = jax.random.normal(key, own.shape[1:], jnp.float32)
    return (own + strength * shared) * lax.rsqrt(1 + strength * strength)


def setup_inputs(seed: int = 0, part: int = 0) -> dict:
    kx, kdy, ka, kb, kz, kf, kh, kl, *keys = jax.random.split(jax.random.key(seed), 8 + 3 * len(NAMES))
    kx, kdy, ka, kb = (jax.random.fold_in(k, part) for k in (kx, kdy, ka, kb))
    kw, km, kv = (keys[i::3] for i in range(3))
    shape = (SEQUENCES, TOKENS, D)
    much_x, much_dy = jax.random.uniform(kz, (2,), jnp.float32, 0.0, 1.0)
    loud = 2.0 ** jax.random.uniform(jax.random.fold_in(kz, 1), (), jnp.float32, -1.0, 2.0)
    layers = 2.0 ** jax.random.uniform(kl, (LAYERS, 1, 1), jnp.float32, -1.0, 1.0)
    x = together(ka, jax.random.normal(kx, shape, jnp.float32), much_x) * bump(kf, D, 4.0)
    dy = together(kb, jax.random.normal(kdy, shape, jnp.float32), much_dy)
    drawn = {"x": x.astype(jnp.bfloat16), "dy": (loud * dy * (SEQUENCES * TOKENS) ** -0.5).astype(jnp.bfloat16)}
    for key, name in zip(kw, NAMES, strict=True):
        w = jax.random.normal(key, SHAPES[name], jnp.float32) * SHAPES[name][1] ** -0.5
        drawn[name] = (w * {"w_gate": 1.0, "w_up": bump(kh, FF, 4.0), "w_down": layers}[name]).astype(jnp.bfloat16)
    for key, name in zip(km, NAMES, strict=True):
        drawn[f"m_{name}"] = 0.1 * jax.random.normal(key, SHAPES[name], jnp.float32)
    for key, name in zip(kv, NAMES, strict=True):
        drawn[f"v_{name}"] = jax.random.uniform(key, SHAPES[name], jnp.float32, 0.005, 0.015)
    return drawn


def matmul(a, w):
    return jnp.dot(a, w, preferred_element_type=jnp.float32).astype(jnp.bfloat16)


def normed(h):
    wide = h.astype(jnp.float32)
    scale = lax.rsqrt(jnp.mean(wide**2, -1, keepdims=True) + 1e-6)
    return (wide * scale).astype(jnp.bfloat16)


def layer(h, w):
    a = normed(h)
    gate = jnp.dot(a, w["w_gate"], preferred_element_type=jnp.float32)
    up = jnp.dot(a, w["w_up"], preferred_element_type=jnp.float32)
    return h + matmul((jax.nn.silu(gate) * up).astype(jnp.bfloat16), w["w_down"])


def adamw(w, m, v, g):
    m = 0.9 * m + 0.1 * g
    v = 0.95 * v + 0.05 * g * g
    step = m * lax.rsqrt(v + 1e-8) + 0.1 * w
    return (w - 0.02 * step).astype(jnp.bfloat16), m, v


def clipped(gradients, sum_of_squares, count):
    factor = jnp.minimum(1.0, 0.5 * lax.rsqrt(sum_of_squares / count + 1e-30))
    return [g * factor for g in gradients]


def stack(weights, h):
    return lax.scan(lambda h, w: (layer(h, w), None), h, weights)[0]


def reference(x, dy, w_gate, w_up, w_down, m_w_gate, m_w_up, m_w_down, v_w_gate, v_w_up, v_w_down):
    weights = dict(zip(NAMES, (w_gate, w_up, w_down), strict=True))

    def take(so_far, sequence):
        h, by_y = sequence
        _, back = jax.vjp(lambda w: stack(w, h), weights)
        return jax.tree.map(lambda total, term: total + term.astype(jnp.float32), so_far, back(by_y)[0]), None

    none_yet = {name: jnp.zeros(w.shape, jnp.float32) for name, w in weights.items()}
    by_weights, _ = lax.scan(take, none_yet, (x, dy))
    gradients = [by_weights[name].astype(jnp.bfloat16).astype(jnp.float32) for name in NAMES]
    gradients = clipped(gradients, sum(jnp.sum(g * g) for g in gradients), sum(g.size for g in gradients))
    new = [
        adamw(w.astype(jnp.float32), m, v, g)
        for w, m, v, g in zip((w_gate, w_up, w_down), (m_w_gate, m_w_up, m_w_down), (v_w_gate, v_w_up, v_w_down), gradients, strict=True)
    ]
    return tuple(one[which] for which in range(3) for one in new)
```

```python
import functools

import jax
import jax.numpy as jnp
from jax import lax
from jax.experimental import pallas as pl
from jax.experimental.pallas import tpu as pltpu
from jax.sharding import PartitionSpec as P

NAMES = ("w_gate", "w_up", "w_down")
F32, BF16 = jnp.float32, jnp.bfloat16
MESH = pl.DeviceIdType.MESH


def matmul(a, w):
    return jnp.dot(a, w, preferred_element_type=F32).astype(BF16)


def normed(h):
    wide = h.astype(F32)
    scale = lax.rsqrt(jnp.mean(wide**2, -1, keepdims=True) + 1e-6)
    return (wide * scale).astype(BF16)


def layer(h, w):
    a = normed(h)
    gate = jnp.dot(a, w["w_gate"], preferred_element_type=F32)
    up = jnp.dot(a, w["w_up"], preferred_element_type=F32)
    return h + matmul((jax.nn.silu(gate) * up).astype(BF16), w["w_down"])


def adamw(w, m, v, g):
    m = 0.9 * m + 0.1 * g
    v = 0.95 * v + 0.05 * g * g
    step = m * lax.rsqrt(v + 1e-8) + 0.1 * w
    return (w - 0.02 * step).astype(BF16), m, v


class Place:
    def __init__(self):
        d = lax.axis_index("dp")
        self.c, self.z, self.y, self.x = d % 2, (d // 2) % 4, (d // 8) % 2, d // 16
        self.own, self.xs, self.ys = self.x * 2 + self.y, (1 - self.x) * 2 + self.y, self.x * 2 + 1 - self.y
        self.diag = (1 - self.x) * 2 + 1 - self.y

    def at(self, plane, z, c):
        return {"dp": (plane * 4 + z) * 2 + c}

    def to_x(self):
        return self.at(self.xs, self.z, self.c)

    def to_y(self):
        return self.at(self.ys, self.z, self.c)

    def to_c(self):
        return self.at(self.own, self.z, 1 - self.c)

    def to_z(self, k):
        return self.at(self.own, (self.z + k) % 4, self.c)

    def partners(self):
        return [self.to_x(), self.to_y(), self.to_c()] + [self.to_z(k) for k in (1, 2, 3)]


def greet(place):
    barrier = pltpu.get_barrier_semaphore()
    for device in place.partners():
        pl.semaphore_signal(barrier, inc=1, device_id=device, device_id_type=MESH)
    pl.semaphore_wait(barrier, 6)


def send(src, dst, send_sem, recv_sem, device):
    pltpu.make_async_remote_copy(src, dst, send_sem, recv_sem, device_id=device, device_id_type=MESH).start()


def await_bytes(ref, sem):
    pltpu.make_async_copy(ref, ref, sem).wait()


class Gather:
    Z, XA, XB, YA, YB, DX, DY, C, OWN, SENT = range(10)
    SEMS = 10

    def __init__(self, place, mine, out, sems):
        self.p, self.mine, self.out, self.sems = place, mine, out, sems

    def along_z(self):
        p = self.p
        here = self.out.at[p.own, p.z, p.c]
        for k in (1, 2, 3):
            send(self.mine, here, self.sems.at[self.SENT], self.sems.at[self.Z], p.to_z(k))
        pltpu.make_async_copy(self.mine, here, self.sems.at[self.OWN]).start()

    def _move(self, plane, zs, slot, device):
        ref = self.out.at[plane, zs, self.p.c]
        send(ref, ref, self.sems.at[self.SENT], self.sems.at[slot], device)

    def _arrived(self, plane, zs, slot):
        await_bytes(self.out.at[plane, zs, self.p.c], self.sems.at[slot])

    def to_plane(self):
        p, lo, hi, al = self.p, pl.ds(0, 2), pl.ds(2, 2), pl.ds(0, 4)
        await_bytes(self.out.at[p.own, pl.ds(0, 3), p.c], self.sems.at[self.Z])
        await_bytes(self.out.at[p.own, p.z, p.c], self.sems.at[self.OWN])
        self._move(p.own, lo, self.XA, p.to_x())
        self._move(p.own, hi, self.YB, p.to_y())
        self._move(p.own, hi, self.XB, p.to_x())
        self._move(p.own, lo, self.YA, p.to_y())
        self._move(p.own, al, self.C, p.to_c())

    def across(self):
        p, lo, hi, al = self.p, pl.ds(0, 2), pl.ds(2, 2), pl.ds(0, 4)
        self._arrived(p.xs, lo, self.XA)
        self._move(p.xs, lo, self.DY, p.to_y())
        self._arrived(p.ys, hi, self.YB)
        self._move(p.ys, hi, self.DX, p.to_x())
        self._arrived(p.xs, hi, self.XB)
        self._move(p.xs, al, self.C, p.to_c())
        self._arrived(p.ys, lo, self.YA)
        self._move(p.ys, al, self.C, p.to_c())

    def to_core(self):
        p = self.p
        self._arrived(p.diag, pl.ds(0, 2), self.DY)
        self._arrived(p.diag, pl.ds(2, 2), self.DX)
        self._move(p.diag, pl.ds(0, 4), self.C, p.to_c())

    def done(self):
        await_bytes(self.out.at[:, :, 0], self.sems.at[self.C])

    def sent(self):
        p = self.p
        for _ in range(3):
            await_bytes(self.mine, self.sems.at[self.SENT])
        for _ in range(7):
            await_bytes(self.out.at[0, :, 0], self.sems.at[self.SENT])


def gather_all(blocks):
    n = len(blocks)
    halves = [(i, half) for i in range(n) for half in range(2)]

    def kernel(*refs):
        ins, outs, held, (load_sem, sems) = refs[:n], refs[n : 2 * n], refs[2 * n : 3 * n], refs[3 * n :]
        place = Place()
        for i in range(n):
            pltpu.make_async_copy(ins[i], held[i], load_sem.at[i]).start()
        greet(place)
        jobs = []
        for j, (i, half) in enumerate(halves):
            w = blocks[i].shape[1] // 2
            cols = pl.ds(half * w, w)
            jobs.append(Gather(place, held[i].at[:, cols], outs[i].at[:, :, :, :, cols], sems.at[j]))
        for j, (i, half) in enumerate(halves):
            if half == 0:
                pltpu.make_async_copy(ins[i], held[i], load_sem.at[i]).wait()
            jobs[j].along_z()
        for s in range(len(jobs) + 2):
            if s < len(jobs):
                jobs[s].to_plane()
            if 0 <= s - 1 < len(jobs):
                jobs[s - 1].across()
            if 0 <= s - 2 < len(jobs):
                jobs[s - 2].to_core()
        for job in jobs:
            job.done()
            job.sent()

    outs = pl.pallas_call(
        kernel,
        name="gather_all",
        in_specs=[pl.BlockSpec(memory_space=pl.ANY)] * n,
        out_specs=[pl.BlockSpec(memory_space=pl.ANY)] * n,
        out_shape=[jax.ShapeDtypeStruct((4, 4, 2) + b.shape, BF16) for b in blocks],
        scratch_shapes=[pltpu.VMEM(b.shape, BF16) for b in blocks]
        + [pltpu.SemaphoreType.DMA((n,)), pltpu.SemaphoreType.DMA((len(halves), Gather.SEMS))],
        compiler_params=pltpu.CompilerParams(collective_id=0, has_side_effects=True),
    )(*blocks)
    return [o.reshape(32 * b.shape[0], b.shape[1]) for o, b in zip(outs, blocks, strict=True)]


def add_into(dst, *srcs):
    n, r, w = dst.shape

    def rows(i, _):
        total = srcs[0][i].astype(F32)
        for s in srcs[1:]:
            total += s[i].astype(F32)
        dst[i] = total.astype(dst.dtype)
        return 0

    for i in range(n):
        rows(i, 0)


class Scatter:
    C, L, P1X, P1Y, XA, XB, YA, YB, Z, SENT = 0, 4, 8, 9, 10, 11, 12, 13, 14, 15
    SEMS = 16

    @staticmethod
    def scratch(r, w):
        return [pltpu.VMEM((4, 4, r, w), BF16), pltpu.VMEM((4, 4, r, w), BF16), pltpu.VMEM((15, r, w), BF16)]

    def __init__(self, place, terms, out, mine, other, arrived, sems):
        self.p, self.terms, self.out, self.mine, self.other, self.sems = place, terms, out, mine, other, sems
        self.p1x, self.p1y = arrived.at[pl.ds(0, 2)], arrived.at[pl.ds(2, 2)]
        self.rx, self.ry, self.rz = arrived.at[pl.ds(4, 4)], arrived.at[pl.ds(8, 4)], arrived.at[pl.ds(12, 3)]

    def start(self):
        p = self.p
        for g, plane in enumerate((p.diag, p.xs, p.ys, p.own)):
            send(self.terms.at[plane, :, 1 - p.c], self.other.at[g], self.sems.at[self.SENT], self.sems.at[self.C + g], p.to_c())
            pltpu.make_async_copy(self.terms.at[plane, :, p.c], self.mine.at[g], self.sems.at[self.L + g]).start()

    def _both(self, g):
        await_bytes(self.other.at[g], self.sems.at[self.C + g])
        await_bytes(self.mine.at[g], self.sems.at[self.L + g])

    def _send(self, src, dst, slot, device):
        send(src, dst, self.sems.at[self.SENT], self.sems.at[slot], device)

    def diagonal(self):
        p, lo, hi = self.p, pl.ds(0, 2), pl.ds(2, 2)
        self._both(0)
        add_into(self.mine.at[0], self.mine.at[0], self.other.at[0])
        self._send(self.mine.at[0, lo], self.p1x, self.P1X, p.to_x())
        self._send(self.mine.at[0, hi], self.p1y, self.P1Y, p.to_y())

    def straight(self):
        p, lo, hi = self.p, pl.ds(0, 2), pl.ds(2, 2)
        self._both(1)
        add_into(self.mine.at[1, lo], self.mine.at[1, lo], self.other.at[1, lo])
        self._send(self.mine.at[1, lo], self.rx.at[lo], self.XA, p.to_x())
        self._both(2)
        add_into(self.mine.at[2, hi], self.mine.at[2, hi], self.other.at[2, hi])
        self._send(self.mine.at[2, hi], self.ry.at[hi], self.YB, p.to_y())

    def joined(self):
        p, lo, hi = self.p, pl.ds(0, 2), pl.ds(2, 2)
        await_bytes(self.p1y, self.sems.at[self.P1Y])
        add_into(self.mine.at[1, hi], self.mine.at[1, hi], self.other.at[1, hi], self.p1y)
        self._send(self.mine.at[1, hi], self.rx.at[hi], self.XB, p.to_x())
        await_bytes(self.p1x, self.sems.at[self.P1X])
        add_into(self.mine.at[2, lo], self.mine.at[2, lo], self.other.at[2, lo], self.p1x)
        self._send(self.mine.at[2, lo], self.ry.at[lo], self.YA, p.to_y())

    def along_z(self):
        p, lo, hi = self.p, pl.ds(0, 2), pl.ds(2, 2)
        self._both(3)
        for part, xs, ys in ((lo, self.XA, self.YA), (hi, self.XB, self.YB)):
            await_bytes(self.rx.at[part], self.sems.at[xs])
            await_bytes(self.ry.at[part], self.sems.at[ys])
            add_into(self.mine.at[3, part], self.mine.at[3, part], self.other.at[3, part], self.rx.at[part], self.ry.at[part])
        for k in (1, 2, 3):
            self._send(self.mine.at[3, (p.z + k) % 4], self.rz.at[k - 1], self.Z, p.to_z(k))

    def last(self):
        await_bytes(self.rz, self.sems.at[self.Z])
        total = self.mine[3, self.p.z].astype(F32)
        for k in range(3):
            total += self.rz[k].astype(F32)
        g = total.astype(BF16)
        self.out[...] = g
        g = g.astype(F32)
        return jnp.sum(g * g)

    def sent(self):
        for _ in range(4):
            await_bytes(self.other.at[0], self.sems.at[self.SENT])
        for _ in range(3):
            await_bytes(self.other.at[0], self.sems.at[self.SENT])
        await_bytes(self.rz, self.sems.at[self.SENT])


def scatter_all(terms):
    n = len(terms)
    shapes = [(t.shape[0] // 32, t.shape[1]) for t in terms]
    halves = [(i, half) for i in range(n) for half in range(2)]
    nj = len(halves)

    def kernel(*refs):
        ins, outs, squares, rest = refs[:n], refs[n : 2 * n], refs[2 * n], refs[2 * n + 1 :]
        bufs, (sums, gone, sums_sem, sems) = rest[: 3 * nj], rest[3 * nj :]
        place = Place()
        greet(place)
        jobs = []
        for j, (i, half) in enumerate(halves):
            w = shapes[i][1] // 2
            cols = pl.ds(half * w, w)
            jobs.append(Scatter(place, ins[i].at[:, :, :, :, cols], outs[i].at[:, cols], *bufs[3 * j : 3 * j + 3], sems.at[j]))
        total = jnp.float32(0)
        for t in range(-2, nj + 2):
            for offset, stage in ((2, Scatter.start), (1, Scatter.diagonal), (1, Scatter.straight), (0, Scatter.joined), (-1, Scatter.along_z)):
                if 0 <= t + offset < nj:
                    stage(jobs[t + offset])
            if 0 <= t - 2 < nj:
                total += jobs[t - 2].last()
        sums[0] = jnp.full((8, 128), total, F32)
        for i, device in enumerate((place.to_c(), place.to_x(), place.to_y())):
            send(sums.at[i], gone.at[i], sums_sem.at[0], sums_sem.at[1 + i], device)
            await_bytes(gone.at[i], sums_sem.at[1 + i])
            sums[i + 1] = sums[i] + gone[i]
        for k in (1, 2, 3):
            send(sums.at[3], gone.at[2 + k], sums_sem.at[0], sums_sem.at[4], place.to_z(k))
        await_bytes(gone.at[pl.ds(3, 3)], sums_sem.at[4])
        squares[...] = (sums[3] + gone[3]) + (gone[4] + gone[5])
        await_bytes(gone, sums_sem.at[0])
        for job in jobs:
            job.sent()

    scratch = []
    for i, _ in halves:
        scratch += Scatter.scratch(shapes[i][0], shapes[i][1] // 2)
    scratch += [pltpu.VMEM((4, 8, 128), F32), pltpu.VMEM((6, 8, 128), F32), pltpu.SemaphoreType.DMA((5,)), pltpu.SemaphoreType.DMA((nj, Scatter.SEMS))]
    *outs, squares = pl.pallas_call(
        kernel,
        name="scatter_all",
        in_specs=[pl.BlockSpec(memory_space=pl.ANY)] * n,
        out_specs=[pl.BlockSpec(memory_space=pltpu.VMEM)] * (n + 1),
        out_shape=[jax.ShapeDtypeStruct(s, BF16) for s in shapes] + [jax.ShapeDtypeStruct((8, 128), F32)],
        scratch_shapes=scratch,
        compiler_params=pltpu.CompilerParams(collective_id=1, has_side_effects=True, vmem_limit_bytes=66_000_000),
    )(*[t.reshape((4, 4, 2) + s) for t, s in zip(terms, shapes, strict=True)])
    return outs, squares


def solution(mesh):
    def step(x, dy, *arrays):
        weights, m, v = (arrays[i : i + 3] for i in (0, 3, 6))
        layers = weights[0].shape[0]
        flat = gather_all([w[number] for number in range(layers) for w in weights])
        full = [dict(zip(NAMES, flat[3 * number : 3 * number + 3], strict=True)) for number in range(layers)]
        h, kept = x[0], []
        for number in range(layers):
            kept.append(h)
            h = layer(h, full[number])
        by_h, terms = dy[0], []
        for number in reversed(range(layers)):
            _, back = jax.vjp(layer, kept[number], full[number])
            by_h, by_w = back(by_h)
            terms += [by_w[name] for name in ("w_down", "w_gate", "w_up")]
        sums, squares = scatter_all(terms)
        sums = {(number, name): sums[3 * (layers - 1 - number) + k] for number in range(layers) for k, name in enumerate(("w_down", "w_gate", "w_up"))}
        gradients = [jnp.stack([sums[number, name] for number in range(layers)]).astype(F32) for name in NAMES]
        count = 32 * sum(g.size for g in gradients)
        factor = jnp.minimum(1.0, 0.5 * lax.rsqrt(squares[0, 0] / count + 1e-30))
        new = [adamw(w.astype(F32), m, v, g * factor) for w, m, v, g in zip(weights, m, v, gradients, strict=True)]
        return tuple(one[which] for which in range(3) for one in new)

    states, cut = P(("rep", "dp"), None, None), P(None, "dp", None)
    return jax.shard_map(
        step,
        mesh=mesh,
        in_specs=(states, states) + (cut,) * 9,
        out_specs=(P("rep", "dp", None),) * 9,
        check_vma=False,
    )
```

```python
import functools

import jax
import jax.numpy as jnp
from jax import lax
from jax.experimental import pallas as pl
from jax.experimental.pallas import tpu as pltpu
from jax.sharding import PartitionSpec as P

F32, BF16 = jnp.float32, jnp.bfloat16
MESH = pl.DeviceIdType.MESH
DEVICES, PLANE, LINE, TILE, LANES = 32, 4, 4, 256, 128
PAIR = 2
LO, HI, ALL = pl.ds(0, PAIR), pl.ds(PAIR, PAIR), pl.ds(0, LINE)
GRID = (PLANE, LINE, PAIR)
LEAD, TOOK, WIRE = 14, 24.0, 25.0
SHARES = ((2, 4, 5), (3, 3, 3, 2)), (2, 3, 3, 3)


def nn(a, b):
    return jnp.dot(a, b, preferred_element_type=F32)


def tn(a, b):
    return lax.dot_general(a, b, (((0,), (0,)), ((), ())), preferred_element_type=F32)


def nt(a, b):
    return lax.dot_general(a, b, (((1,), (1,)), ((), ())), preferred_element_type=F32)


def norm_scale(wide):
    return lax.rsqrt(jnp.mean(wide * wide, -1, keepdims=True) + 1e-6)


def norm_rows(h):
    wide = h.astype(F32)
    return (wide * norm_scale(wide)).astype(BF16)


def norm_back(da, h):
    wide, da = h.astype(F32), da.astype(F32)
    scale = norm_scale(wide)
    return (da * scale - wide * (scale * scale * scale * jnp.mean(da * wide, -1, keepdims=True))).astype(BF16)


def silu_back(gate, up, by_act):
    s = jax.nn.sigmoid(gate)
    return (by_act * up * s * (1 + gate * (1 - s))).astype(BF16), (by_act * gate * s).astype(BF16)


class Place:
    def __init__(self):
        d = lax.axis_index("dp")
        self.c, chip = d % PAIR, d // PAIR
        self.z, self.own = chip % LINE, chip // LINE
        x, y = self.own // PAIR, self.own % PAIR
        self.xs, self.ys, self.diag = (1 - x) * PAIR + y, x * PAIR + 1 - y, (1 - x) * PAIR + 1 - y
        self.near, self.far = pl.ds(self.z // PAIR * PAIR, PAIR), pl.ds(PAIR - self.z // PAIR * PAIR, PAIR)
        self.inner = jnp.logical_or(self.z == 1, self.z == 2)
        self.outer = jnp.logical_not(self.inner)
        at = lambda plane, z, c: {"dp": (plane * LINE + z) * PAIR + c}
        self.to_x, self.to_y, self.to_diag = (at(plane, self.z, self.c) for plane in (self.xs, self.ys, self.diag))
        self.to_c = at(self.own, self.z, 1 - self.c)
        self.to_z = [at(self.own, (self.z + k) % LINE, self.c) for k in range(1, LINE)]
        self.next_z = at(self.own, self.z + 1 - PAIR * (self.z % PAIR), self.c)
        self.across_z = at(self.own, LINE - 1 - self.z, self.c)
        self.sharers = [self.to_x, self.to_y, self.to_c, *self.to_z]


def signal_all(sem, devices):
    for device in devices:
        pl.semaphore_signal(sem, inc=1, device_id=device, device_id_type=MESH)


def greet(devices):
    barrier = pltpu.get_barrier_semaphore()
    signal_all(barrier, devices)
    pl.semaphore_wait(barrier, len(devices))


def send(src, dst, send_sem, recv_sem, device):
    pltpu.make_async_remote_copy(src, dst, send_sem, recv_sem, device_id=device, device_id_type=MESH).start()


def await_bytes(ref, sem):
    pltpu.make_async_copy(ref, ref, sem).wait()


class Gather:
    Z, Z2, Z3, XA, XB, YA, YB, DX, DY, C, OWN, SENT = SLOTS = range(12)

    def __init__(self, place, mine, blocks, amount, sems, direct):
        self.p, self.mine, self.blocks, self.amount, self.sems, self.direct = place, mine, blocks, amount, sems, direct

    def z_first(self):
        p = self.p
        (here,) = self.blocks(p.own, p.z, p.c)
        pltpu.make_async_copy(self.mine, here, self.sems.at[self.OWN]).start()
        for device in p.to_z if self.direct else [p.next_z]:
            send(self.mine, here, self.sems.at[self.SENT], self.sems.at[self.Z], device)

    def _move(self, plane, zs, slot, device):
        for ref in self.blocks(plane, zs, self.p.c):
            send(ref, ref, self.sems.at[self.SENT], self.sems.at[slot], device)

    def _wait(self, slot, blocks=PAIR):
        await_bytes(self.amount(blocks), self.sems.at[slot])

    def z_second(self):
        @pl.when(self.p.inner)
        def _():
            self._wait(self.Z, 1)
            self._wait(self.OWN, 1)
            self._move(self.p.own, self.p.near, self.Z2, self.p.across_z)

    def z_third(self):
        @pl.when(self.p.inner)
        def _():
            self._wait(self.Z2)
            self._move(self.p.own, self.p.far, self.Z3, self.p.next_z)

    def plane(self):
        p = self.p
        if self.direct:
            self._wait(self.Z, LINE - 1)
            self._wait(self.OWN, 1)
        else:

            @pl.when(p.outer)
            def _():
                self._wait(self.Z, 1)
                self._wait(self.OWN, 1)
                self._wait(self.Z3)

        self._move(p.own, LO, self.XA, p.to_x)
        self._move(p.own, HI, self.YB, p.to_y)
        self._move(p.own, HI, self.XB, p.to_x)
        self._move(p.own, LO, self.YA, p.to_y)
        self._move(p.own, ALL, self.C, p.to_c)

    def across(self):
        p = self.p
        self._wait(self.XA)
        self._move(p.xs, LO, self.DY, p.to_y)
        self._wait(self.YB)
        self._move(p.ys, HI, self.DX, p.to_x)

    def to_core(self):
        p = self.p
        self._wait(self.XB)
        self._move(p.xs, ALL, self.C, p.to_c)
        self._wait(self.YA)
        self._move(p.ys, ALL, self.C, p.to_c)

    def last_to_core(self):
        self._wait(self.DY)
        self._wait(self.DX)
        self._move(self.p.diag, ALL, self.C, self.p.to_c)

    def done(self):
        self._wait(self.C, PLANE * LINE)

    def sent(self):
        for _ in range(LINE - 1 if self.direct else 1):
            await_bytes(self.mine, self.sems.at[self.SENT])
        if not self.direct:
            pl.when(self.p.inner)(functools.partial(self._wait, self.SENT, LINE))
        for _ in range(7):
            self._wait(self.SENT, LINE)


def add_into(dst, *srcs):
    def one(i, _):
        for z in range(dst.shape[1]):
            total = srcs[0][i, z].astype(F32)
            for s in srcs[1:]:
                total += s[i, z].astype(F32)
            dst[i, z] = total.astype(dst.dtype)
        return 0

    if dst.shape[0] == 1:
        one(0, 0)
    else:
        lax.fori_loop(0, dst.shape[0], one, 0)


class Scatter:
    P1X, P1Y, XA, XB, YA, YB, Z, SENT, *C, L0, L1, L2, L3 = SLOTS = range(16)
    L = (L0, L1, L2, L3)

    @staticmethod
    def scratch(n, r, w):
        return [pltpu.VMEM(s + (r, w), BF16) for s in ((PLANE, n, LINE), (PLANE, n, LINE), (n, 3 * LINE), (LINE - 1, n))]

    def __init__(self, place, n, terms, out, slot, sems, acc):
        self.p, self.n, self.terms, self.out, self.sems, self.acc = place, n, terms, out, sems, acc
        mine, other, arrived, rz = slot
        some = pl.ds(0, n)
        self.mine, self.other = (lambda g, zs=ALL: mine.at[g, some, zs]), (lambda g, zs=ALL: other.at[g, some, zs])
        self.p1x, self.p1y = arrived.at[some, LO], arrived.at[some, HI]
        self.rx, self.ry = (lambda lo: arrived.at[some, pl.ds(LINE + lo, PAIR)]), (lambda lo: arrived.at[some, pl.ds(PAIR * LINE + lo, PAIR)])
        self.rz, self.kept = rz.at[:, some], mine

    def start(self):
        p = self.p
        for g, plane in enumerate((p.diag, p.xs, p.ys, p.own)):
            for ref, part in self.terms(plane, 1 - p.c):
                send(ref, part(self.other(g)), self.sems.at[self.SENT], self.sems.at[self.C[g]], p.to_c)
            for ref, part in self.terms(plane, p.c):
                pltpu.make_async_copy(ref, part(self.mine(g)), self.sems.at[self.L[g]]).start()

    def _both(self, g):
        await_bytes(self.other(g), self.sems.at[self.C[g]])
        await_bytes(self.mine(g), self.sems.at[self.L[g]])

    def _send(self, src, dst, slot, device):
        send(src, dst, self.sems.at[self.SENT], self.sems.at[slot], device)

    def diagonal(self):
        p = self.p
        self._both(0)
        add_into(self.mine(0), self.mine(0), self.other(0))
        self._send(self.mine(0, LO), self.p1x, self.P1X, p.to_x)
        self._send(self.mine(0, HI), self.p1y, self.P1Y, p.to_y)

    def straight(self):
        p = self.p
        self._both(1)
        add_into(self.mine(1, LO), self.mine(1, LO), self.other(1, LO))
        self._send(self.mine(1, LO), self.rx(0), self.XA, p.to_x)
        self._both(2)
        add_into(self.mine(2, HI), self.mine(2, HI), self.other(2, HI))
        self._send(self.mine(2, HI), self.ry(PAIR), self.YB, p.to_y)

    def joined(self):
        p = self.p
        await_bytes(self.p1y, self.sems.at[self.P1Y])
        add_into(self.mine(1, HI), self.mine(1, HI), self.other(1, HI), self.p1y)
        self._send(self.mine(1, HI), self.rx(PAIR), self.XB, p.to_x)
        await_bytes(self.p1x, self.sems.at[self.P1X])
        add_into(self.mine(2, LO), self.mine(2, LO), self.other(2, LO), self.p1x)
        self._send(self.mine(2, LO), self.ry(0), self.YA, p.to_y)

    def along_z(self):
        p = self.p
        self._both(3)
        for part, lo, xs, ys in ((LO, 0, self.XA, self.YA), (HI, PAIR, self.XB, self.YB)):
            await_bytes(self.rx(lo), self.sems.at[xs])
            await_bytes(self.ry(lo), self.sems.at[ys])
            add_into(self.mine(3, part), self.mine(3, part), self.other(3, part), self.rx(lo), self.ry(lo))
        for k, device in enumerate(p.to_z):
            self._send(self.mine(3, (p.z + 1 + k) % LINE), self.rz.at[k], self.Z, device)

    def last(self):
        await_bytes(self.rz, self.sems.at[self.Z])
        for i in range(self.n):
            total = self.kept[3, i, self.p.z].astype(F32)
            for k in range(LINE - 1):
                total += self.rz[k, i].astype(F32)
            g = total.astype(BF16)
            self.out(i)[:] = g
            g = g.astype(F32)
            g = g * g
            r, w = g.shape
            lanes = g[:, :LANES]
            for k in range(1, w // LANES):
                lanes += g[:, LANES * k : LANES * (k + 1)]
            self.acc[:] += jnp.sum(lanes.reshape(-1, *self.acc.shape), 0)

    def sent(self):
        for _ in range(7):
            await_bytes(self.other(0), self.sems.at[self.SENT])
        await_bytes(self.rz, self.sems.at[self.SENT])


class Pump:
    def __init__(self):
        self.items, self.now = [], 0.0

    def insert(self, when, act, tag=None):
        at = len(self.items)
        while at and self.items[at - 1][0] > when:
            at -= 1
        self.items.insert(at, (when, act, tag))

    def due(self):
        acts = []
        while self.items and self.items[0][0] <= self.now:
            acts.append(self.items.pop(0)[1])
        return acts

    def through(self, tag):
        acts = []
        while any(t == tag for _, _, t in self.items):
            when, act, _ = self.items.pop(0)
            self.now = max(self.now, when)
            acts.append(act)
        return acts

    def plan(self, steps, cost, gates=None, inject=None):
        ticks = {}
        for s in range(steps):
            self.now += cost
            if inject and s in inject:
                for put in inject[s]:
                    put()
            acts = self.due()
            if gates and s + 1 in gates:
                acts += self.through(gates[s + 1])
            if acts:
                ticks[s] = acts
        return ticks


def run(acts):
    for act in acts:
        act()


def stream(steps, ins, outs, body, ticks, late=(), before=None):
    def fetch(step):
        for where, buf, sem in ins:
            pltpu.make_async_copy(where(step), buf.at[step % PAIR], sem.at[step % PAIR]).start()

    def one(step, _):
        slot = step % PAIR
        early = step + 1 < steps
        for t in late:
            early = jnp.logical_and(early, step != t)
        pl.when(early)(lambda: fetch(step + 1))
        for _, buf, sem in ins:
            await_bytes(buf.at[slot], sem.at[slot])
        body(step, [buf.at[slot] for _, buf, _ in ins], [buf.at[slot] for _, buf, _ in outs])

        @pl.when(step >= 1)
        def _():
            for _, buf, sem in outs:
                await_bytes(buf.at[1 - slot], sem.at[1 - slot])

        for where, buf, sem in outs:
            pltpu.make_async_copy(buf.at[slot], where(step), sem.at[slot]).start()
        for t, acts in plan.items():
            pl.when(step == t)(functools.partial(run, acts))
        for t in late:
            pl.when(step == t)(lambda t=t: fetch(t + 1))
        return 0

    fetch(0)
    if before is not None:
        before()
    plan = ticks()
    lax.fori_loop(0, steps, one, 0)
    for _, buf, sem in outs:
        await_bytes(buf.at[(steps - 1) % PAIR], sem.at[(steps - 1) % PAIR])


def cols(step, width):
    return pl.ds(pl.multiple_of(step * width, width), width)


def cuts(total, *shares):
    whole, at, parts = sum(shares), 0, []
    for k in range(len(shares)):
        end = -(-total * sum(shares[: k + 1]) // whole)
        if end > at:
            parts.append((at, end - at))
        at = end
    return parts


def concat(ref, n):
    return jnp.concatenate([ref[j] for j in range(n)], axis=-1)


shape = jax.ShapeDtypeStruct
any_, whole = pl.BlockSpec(memory_space=pl.ANY), pl.BlockSpec(memory_space=pltpu.VMEM)


def two(*dims, dtype=BF16):
    return pltpu.VMEM((PAIR, *dims), dtype)


class Sizes:
    def __init__(self, tokens, d, ff):
        self.tokens, self.d, self.ff, self.half = tokens, d, ff, d // PAIR
        self.tiles, self.rd, self.rf = ff // TILE, d // DEVICES, ff // DEVICES
        self.parts = cuts(self.tiles, *SHARES[1])
        self.deep, self.tall, self.wide = (self.tiles, *GRID, self.rd, TILE), (ff, d), (self.tiles, tokens, TILE)
        self.thin, self.turned = (tokens, d), (d, tokens)
        self.blocks = [shape((self.rd, ff), BF16)] * PAIR + [shape((self.rf, d), BF16)]
        slots = Scatter.scratch(1, self.rf, self.half) * PAIR
        for _, size in self.parts:
            slots += Scatter.scratch(size, self.rd, TILE) * PAIR
        self.n_slots = PAIR + PAIR * len(self.parts)
        self.slot_size, self.slots = len(slots) // self.n_slots, slots
        many = PAIR if tokens % (PAIR * LINE * TILE) == 0 else 1
        self.halves = [pl.ds(q * (tokens // many), tokens // many) for q in range(many)]
        self.hidden_bufs = [two(tokens, TILE, dtype=F32)] * PAIR + [two(TILE, d)] + [two(tokens, TILE)] * PAIR
        self.hidden_bufs += [two(*GRID, self.rd, TILE)] * PAIR + [two(TILE, d)]


def block_rows(plane, z, c, r):
    return pl.ds(pl.multiple_of(((plane * LINE + z) * PAIR + c) * r, 8), r)


def piece(refs, bufs, sems):
    return [(lambda s, ref=ref: ref.at[s], buf, sems.at[k]) for k, (ref, buf) in enumerate(zip(refs, bufs, strict=True))]


def scatters(place, pump, size, slots, sems, acc, out, down, wide):
    state = {"free": 0.0}

    def scatter(n, terms, to, slot, share):
        one = Scatter(place, n, terms, to, slots[slot], sems.at[slot], acc)
        wire = WIRE * share

        def put():
            now = pump.now
            start = max(now + 3, state["free"])
            state["free"] = start + wire
            ahead, end = max(now + 3, start - 4), start + 1.6 * wire + 5
            acts = [(now, one.start), (ahead, one.diagonal), (ahead, one.straight), (start + 0.4 * wire, one.joined)]
            acts += [(start + wire + 2, one.along_z), (end, one.last), (end, one.sent)]
            for when, act in acts:
                pump.insert(when, act)

        return put

    def down_job(k):
        part = pl.ds(k * size.half, size.half)
        terms = lambda plane, c: [(down.at[block_rows(plane, z, c, size.rf), part], lambda to, z=z: to.at[0, z]) for z in range(LINE)]
        return scatter(1, terms, lambda i: out[-1].at[:, part], k, 0.5)

    def wide_job(b, k):
        start, n = size.parts[b]
        terms = lambda plane, c: [(wide[k].at[pl.ds(start, n), plane, :, c], lambda to: to)]
        to = lambda i: out[k].at[:, pl.ds((start + i) * TILE, TILE)]
        return scatter(n, terms, to, PAIR + PAIR * b + k, n / size.tiles)

    jobs = [[down_job(k) for k in range(PAIR)]] + [[wide_job(b, k) for k in range(PAIR)] for b in range(len(size.parts))]

    def put_all(puts):
        for put in puts:
            put()

    return [functools.partial(put_all, puts) for puts in jobs]


def hidden(size, pump, by, at, ins, grads, kept, puts, cost, before, sems, gbuf, ubuf, wdbuf, dgbuf, dubuf, gout, uout, wbuf):
    in_sem, out_sem = sems
    gate, up, w_down = ins

    def body(step, ins, outs):
        dg, du = outs[PAIR:] if kept else (dgbuf.at[0], dubuf.at[0])
        for part in size.halves:
            by_act = nt(by[part, :], ins[2][:]).astype(BF16).astype(F32)
            dg[part, :], du[part, :] = silu_back(ins[0][part, :], ins[1][part, :], by_act)
        for out, grad in zip(outs, (dg, du)):
            out[:] = nn(at[:], grad[:]).astype(BF16).reshape(*GRID, size.rd, TILE)

    outs = piece((*grads, *kept), (gout, uout, dgbuf, dubuf)[: PAIR + len(kept)], out_sem)
    inject = {min(start + n, size.tiles - 1): [put] for (start, n), put in zip(size.parts, puts[:-1])}
    streams = piece((gate, up), (gbuf, ubuf), in_sem)
    streams.append((lambda s: w_down.at[cols(s, TILE), :], wdbuf, in_sem.at[2]))
    before = before and functools.partial(before, dgbuf, wbuf)
    stream(size.tiles, streams, outs, body, lambda: pump.plan(size.tiles, cost, inject=inject), before=before)
    puts[-1]()
    run(pump.due())


def first_part(x, dy, weights):
    size = Sizes(*x.shape, weights[0].shape[-1])
    tokens, d, ff, tiles, rd, rf, half = size.tokens, size.d, size.ff, size.tiles, size.rd, size.rf, size.half
    rows, few = tokens // LINE, tokens // (PAIR * LINE)
    chunks = [cuts(tiles, *shares) for shares in SHARES[0]]
    jobs_of, gates = [], [{}, {}]
    for layer in range(PAIR):
        for start, n in chunks[layer]:
            if layer and start == chunks[1][-1][0]:
                jobs_of.append((1, 2, 0, half))
            jobs_of += [(layer, 0, start, n), (layer, 1, start, n)]
            gates[layer][start] = len(jobs_of) - 1
        jobs_of += [(1, 2, half, half)] if layer else [(0, 2, 0, half), (0, 2, half, half)]
        gates[layer]["down"] = len(jobs_of) - 1
    nj = len(jobs_of)
    held_shapes = [(PAIR, tiles, rd, TILE), (PAIR, tiles, rd, TILE), (PAIR, rf, d)]
    deep, tall, wide, thin, turned = size.deep, size.tall, size.wide, size.thin, size.turned
    hbm = [turned, wide, deep, deep, tall, deep, deep, tall, thin, tall, wide, wide, deep, deep]
    hbm = [shape(thin, BF16), shape(tall, BF16), shape(wide, F32), shape(wide, F32)] + [shape(dims, BF16) for dims in hbm]
    hbm += [shape(wide, F32)] * PAIR
    scratch = [pltpu.VMEM(dims, BF16) for dims in held_shapes + [thin, thin, turned, deep]]

    def kernel(*refs):
        it = iter(refs)
        take = lambda n: [next(it) for _ in range(n)]
        x_hbm, dy_hbm, *w_hbm = take(PAIR + len(weights))
        *out, acc = take(len(weights) + 1)
        dh1, _, gate0, up0, a0t, act0, g0, u0, d0, g1, u1, d1, h1_hbm, dwd1, dg1, du1, dwg1, dwu1, gate1, up1 = take(len(hbm))
        full = [[g0, u0, d0], [g1, u1, d1]]
        *held, a, by, at, wg = take(len(scratch))
        slots = [take(size.slot_size) for _ in range(size.n_slots)]
        load_sem, ag_sems, rs_sems, in_sem, out_sem, one_sem = take(6)
        s_x, s_at, s_w, s_u = (one_sem.at[k] for k in range(4))
        place = Place()

        def load(k, layer):
            ref, sem = w_hbm[k].at[layer], load_sem.at[k, layer]
            if k == PAIR:
                pltpu.make_async_copy(ref, held[k].at[layer], sem).start()
            else:
                for t in range(tiles):
                    pltpu.make_async_copy(ref.at[:, pl.ds(TILE * t, TILE)], held[k].at[layer, t], sem).start()

        x_load = pltpu.make_async_copy(x_hbm, by, s_x)
        for layer in range(PAIR):
            for k in range(len(held)):
                load(k, layer)
                if k == 1 and not layer:
                    x_load.start()
        greet(place.sharers)
        acc[:] = jnp.zeros_like(acc)
        pump, jobs, loaded = Pump(), [], set()

        def first(j):
            layer, k, _, _ = jobs_of[j]
            if (k, layer) not in loaded:
                await_bytes(held[k].at[layer], load_sem.at[k, layer])
                loaded.add((k, layer))
            jobs[j].z_first()

        clock = begun = 4.0
        for j, (layer, k, start, n) in enumerate(jobs_of):
            part, ref = pl.ds(start, n), full[layer][k]
            if k == PAIR:

                def blocks(plane, zs, c, ref=ref, part=part):
                    zs = [zs.start + i for i in range(zs.size)] if isinstance(zs, pl.Slice) else [zs]
                    return [ref.at[block_rows(plane, z, c, rf), part] for z in zs]

                amount = lambda n, ref=ref, part=part: ref.at[pl.ds(0, n * rf), part]
                mine = held[k].at[layer, :, part]
            else:
                blocks = lambda plane, zs, c, ref=ref, part=part: [ref.at[part, plane, zs, c]]
                amount = lambda n, ref=ref, part=part: ref.at[part, pl.ds(0, max(1, n // LINE)), pl.ds(0, min(n, LINE)), 0]
                mine = held[k].at[layer, part]
            job = Gather(place, mine, blocks, amount, ag_sems.at[j], j < PAIR)
            jobs.append(job)
            took = TOOK * n / (d if k == PAIR else tiles)
            unit = took / 6
            lead = min(max(0.33 * clock - 5, 3), LEAD)
            zero = begun - 4
            pump.insert(zero, functools.partial(first, j))
            if not job.direct:
                pump.insert(zero + unit + 2.5, job.z_second)
                pump.insert(zero + 3 * unit + 5, job.z_third)
            ready = max(zero + 5 * unit + (5 if job.direct else 7.5), clock - lead)
            clock = max(clock, ready)
            pump.insert(ready, job.plane)
            pump.insert(clock + 0.4 * took, job.across)
            pump.insert(clock + 0.75 * took, job.to_core)
            behind = PAIR if j >= nj - 3 else lead
            pump.insert(clock + took + behind + 1, job.last_to_core)
            pump.insert(clock + took + behind + 2, job.done, j)
            clock += took
            begun += (0.5 if j > 1 else 0.2) * took
        pump.now = 3.0
        run(pump.due())
        x_load.wait()
        a0_out = pltpu.make_async_copy(at, a0t, s_at)
        dy_load = pltpu.make_async_copy(dy_hbm, by, s_x)

        step = min(TILE, tokens)

        def norm(i, _):
            part = cols(i, step)
            normed = norm_rows(by[part, :])
            a[part, :] = normed
            at[:, part] = normed.T
            return 0

        lax.fori_loop(0, tokens // step, norm, 0)
        a0_out.start()
        pump.now = 8.0

        def gate_up(layer, gate, up, before, wgate, wup, gbuf, ubuf, actbuf, dwbuf):
            def body(step, ins, outs):
                g = nn(a[:], ins[0][:].reshape(d, TILE))
                u = nn(a[:], ins[1][:].reshape(d, TILE))
                outs[0][:] = g
                outs[1][:] = u
                product = (g * jax.nn.sigmoid(g) * u).astype(BF16)
                if layer:
                    actbuf[0] = product
                    outs[2][:] = tn(actbuf[0], by[:]).astype(BF16)
                else:
                    outs[2][:] = product

            run(pump.through(gates[layer][0]))
            later = {s: j for s, j in gates[layer].items() if s in range(1, tiles)}
            outs = piece((gate, up, act0), (gbuf, ubuf, actbuf), out_sem)
            if layer:
                outs[-1] = (lambda s: dwd1.at[cols(s, TILE), :], dwbuf, out_sem.at[2])
            stream(
                tiles,
                piece(full[layer][:PAIR], (wgate, wup), in_sem),
                outs,
                body,
                lambda: pump.plan(tiles, 3.7 if layer else 2.5, later),
                late=[s - 1 for s in later],
                before=before,
            )

        def down(wd, tall, hbuf):
            run(pump.through(gates[0]["down"]))
            wd_load = pltpu.make_async_copy(d0, wd, s_w)
            wd_load.start()

            def ready():
                a0_out.wait()
                wd_load.wait()

            def body(step, ins, outs):
                part = cols(step, rows)
                h = by[part, :] + nn(concat(ins[0], tiles), wd[:]).astype(BF16)
                outs[0][:] = h
                normed = norm_rows(h)
                a[part, :] = normed
                at[:, part] = normed.T

            stream(
                tokens // rows,
                [(lambda s: act0.at[:, cols(s, rows), :], tall, in_sem.at[0])],
                [(lambda s: h1_hbm.at[cols(s, rows), :], hbuf, out_sem.at[0])],
                body,
                lambda: pump.plan(tokens // rows, 3.8),
                before=ready,
            )
            dy_load.start()

        tile_bufs = [two(*GRID, rd, TILE)] * PAIR + [two(tokens, TILE, dtype=F32)] * PAIR + [two(tokens, TILE), two(TILE, d)]
        pl.run_scoped(functools.partial(gate_up, 0, gate0, up0, None), *tile_bufs)
        pl.run_scoped(down, pltpu.VMEM(d0.shape, BF16), two(tiles, rows, TILE), two(rows, d))
        pl.run_scoped(functools.partial(gate_up, 1, gate1, up1, dy_load.wait), *tile_bufs)
        run(pump.through(nj - 1))
        assert not pump.items
        put_down, *put_wide = scatters(place, pump, size, slots, rs_sems, acc, out, dwd1, (dwg1, dwu1))
        put_down()
        run(pump.due())
        wg_load = pltpu.make_async_copy(g1, wg, s_w)
        wg_load.start()
        ins, grads = (gate1, up1, d1), (dwg1, dwu1)
        pl.run_scoped(
            functools.partial(hidden, size, pump, by, at, ins, grads, (dg1, du1), put_wide, 4.4, None, (in_sem, out_sem)), *size.hidden_bufs
        )

        def states(wu, dgbuf, dubuf, hbuf):
            wu_load = pltpu.make_async_copy(u1, wu, s_u)
            wu_load.start()

            def ready():
                wg_load.wait()
                wu_load.wait()

            def body(step, ins, outs):
                part = cols(step, few)
                dg, du, h = (ref for ref in ins)
                da = nt(concat(dg, tiles), concat(wg, tiles).reshape(d, ff)) + nt(concat(du, tiles), concat(wu, tiles).reshape(d, ff))
                by[part, :] = by[part, :] + norm_back(da.astype(BF16), h[:])

            ins = [(lambda s, ref=ref: ref.at[:, cols(s, few), :], buf, in_sem.at[k]) for k, (ref, buf) in enumerate(((dg1, dgbuf), (du1, dubuf)))]
            ins.append((lambda s: h1_hbm.at[cols(s, few), :], hbuf, in_sem.at[2]))
            stream(tokens // few, ins, [], body, lambda: pump.plan(tokens // few, 3.6), before=ready)

        pl.run_scoped(states, pltpu.VMEM(wg.shape, BF16), two(tiles, few, TILE), two(tiles, few, TILE), two(few, d))
        by_out = pltpu.make_async_copy(by, dh1, s_x)
        by_out.start()
        pump.now = 1e9
        run(pump.due())
        for job in jobs:
            job.sent()
        by_out.wait()

    DMA = pltpu.SemaphoreType.DMA
    outs = pl.pallas_call(
        kernel,
        name="first_part",
        in_specs=[any_] * (PAIR + len(weights)),
        out_specs=[whole] * (len(weights) + 1) + [any_] * len(hbm),
        out_shape=size.blocks + [shape((8, LANES), F32)] + hbm,
        scratch_shapes=scratch
        + size.slots
        + [DMA((3, PAIR)), DMA((nj, len(Gather.SLOTS))), DMA((size.n_slots, len(Scatter.SLOTS)))]
        + [DMA((4, PAIR)), DMA((4, PAIR)), DMA((4,))],
        compiler_params=pltpu.CompilerParams(collective_id=0, has_side_effects=True, vmem_limit_bytes=66_500_000),
    )(x, dy, *weights)
    *sums, acc = outs[: len(weights) + 1]
    dh1, _, gate0, up0, a0t, act0, _, _, d0 = outs[len(weights) + 1 :][:9]
    return sums, acc, (dh1, gate0, up0, a0t, act0, d0)


def second_part(last_acc, dh1, gate0, up0, a0t, act0, d0):
    size = Sizes(*dh1.shape, d0.shape[0])
    deep, tall = shape(size.deep, BF16), shape(size.tall, BF16)
    n = len(size.blocks)

    def kernel(*refs):
        it = iter(refs)
        take = lambda n: [next(it) for _ in range(n)]
        acc_in, dh1_hbm, gate0, up0, a0t, act0, d0 = take(7)
        *out, squares = take(n + 1)
        dwd0, dwg0, dwu0 = take(n)
        by, at = take(PAIR)
        slots = [take(size.slot_size) for _ in range(size.n_slots)]
        acc, sums, gone, rs_sems, in_sem, out_sem, sums_sem, one_sem = take(8)
        place, pump = Place(), Pump()
        by_load, at_load = pltpu.make_async_copy(dh1_hbm, by, one_sem.at[0]), pltpu.make_async_copy(a0t, at, one_sem.at[1])
        by_load.start()

        def between(abuf, wbuf):
            at_load.start()

            def ready():
                greet(place.sharers)
                acc[:] = acc_in[:]
                by_load.wait()

            def body(step, ins, outs):
                outs[0][:] = tn(ins[0][:], by[:]).astype(BF16)

            outs = [(lambda s: dwd0.at[cols(s, TILE), :], wbuf, out_sem.at[3])]
            stream(size.tiles, piece((act0,), (abuf,), in_sem.at[pl.ds(3, 1)]), outs, body, dict, before=ready)
            put_down()
            run(pump.due())
            at_load.wait()

        put_down, *put_wide = scatters(place, pump, size, slots, rs_sems, acc, out, dwd0, (dwg0, dwu0))
        ins, grads = (gate0, up0, d0), (dwg0, dwu0)
        pl.run_scoped(
            functools.partial(hidden, size, pump, by, at, ins, grads, (), put_wide, 3.9, between, (in_sem, out_sem)), *size.hidden_bufs
        )
        pump.now = 1e9
        run(pump.due())
        sums[0] = jnp.full(acc.shape, jnp.sum(acc[:]), F32)
        hops = [[place.to_c], [place.to_x, place.to_y, place.to_diag], place.to_z]
        at_gone = 0
        for k, devices in enumerate(hops):
            for i, device in enumerate(devices):
                send(sums.at[k], gone.at[at_gone + i], sums_sem.at[len(hops)], sums_sem.at[k], device)
            await_bytes(gone.at[pl.ds(at_gone, len(devices))], sums_sem.at[k])
            total = sums[k]
            for i in range(len(devices)):
                total += gone[at_gone + i]
            at_gone += len(devices)
            if k < len(hops) - 1:
                sums[k + 1] = total
            else:
                squares[:] = total
        await_bytes(gone, sums_sem.at[len(hops)])

    DMA = pltpu.SemaphoreType.DMA
    tile = (8, LANES)
    *sums, squares = pl.pallas_call(
        kernel,
        name="second_part",
        in_specs=[whole] + [any_] * 6,
        out_specs=[whole] * (n + 1) + [any_] * n,
        out_shape=size.blocks + [shape(tile, F32)] + [tall, deep, deep],
        scratch_shapes=[pltpu.VMEM(size.thin, BF16), pltpu.VMEM(size.turned, BF16)]
        + size.slots
        + [pltpu.VMEM(tile, F32), pltpu.VMEM((3, *tile), F32), pltpu.VMEM((7, *tile), F32)]
        + [DMA((size.n_slots, len(Scatter.SLOTS))), DMA((4, PAIR)), DMA((4, PAIR)), DMA((4,)), DMA((PAIR,))],
        compiler_params=pltpu.CompilerParams(collective_id=1, has_side_effects=True, vmem_limit_bytes=66_500_000),
    )(last_acc, dh1, gate0, up0, a0t, act0, d0)[: n + 1]
    return sums, squares


def adamw(weights, m, v, sums, squares):
    n = len(weights)
    count = DEVICES * sum(w.size for w in weights)

    def kernel(squares_ref, *refs):
        factor = jnp.minimum(1.0, 0.5 * lax.rsqrt(squares_ref[:1, :1] / count + 1e-30))
        for k in range(n):
            w, m, v, g, last_g, new_w, new_m, new_v = refs[k::n]
            grad = jnp.where(pl.program_id(0) == 0, g[:].astype(F32), last_g[:].astype(F32)) * factor
            m_next = 0.9 * m[0] + 0.1 * grad
            v_next = 0.95 * v[0] + 0.05 * grad * grad
            wide = w[0].astype(F32)
            new_w[0] = (wide - 0.02 * (m_next * lax.rsqrt(v_next + 1e-8) + 0.1 * wide)).astype(BF16)
            new_m[0] = m_next
            new_v[0] = v_next

    blocks = [pl.BlockSpec((1, *w.shape[1:]), lambda layer: (layer, 0, 0)) for w in weights]
    once = [pl.BlockSpec(s.shape, lambda layer: (0, 0)) for s in (squares, *sums)]
    return pl.pallas_call(
        kernel,
        name="adamw",
        grid=(PAIR,),
        in_specs=once[:1] + blocks * 3 + once[1:],
        out_specs=blocks * 3,
        out_shape=[shape(w.shape, BF16) for w in weights] + [shape(w.shape, F32) for w in weights] * PAIR,
    )(squares, *weights, *m, *v, *sums)


def solution(mesh):
    def step(x, dy, *arrays):
        weights, m, v = (arrays[3 * i : 3 * i + 3] for i in range(3))
        last, acc, kept = first_part(x[0], dy[0], weights)
        sums, squares = second_part(acc, *kept)
        return tuple(adamw(weights, m, v, [*sums, *last], squares))

    states, cut = P(("rep", "dp"), None, None), P(None, "dp", None)
    return jax.shard_map(
        step,
        mesh=mesh,
        in_specs=(states, states) + (cut,) * 9,
        out_specs=(P("rep", "dp", None),) * 9,
        check_vma=False,
    )
```

```python
import functools

import jax
import jax.numpy as jnp
from jax import lax
from jax.experimental import pallas as pl
from jax.experimental.pallas import tpu as pltpu
from jax.sharding import PartitionSpec as P

F32, BF16 = jnp.float32, jnp.bfloat16
MESH = pl.DeviceIdType.MESH
DEVICES, PLANE, LINE, TILE, LANES = 32, 4, 4, 256, 128
PAIR = 2
LO, HI, ALL = pl.ds(0, PAIR), pl.ds(PAIR, PAIR), pl.ds(0, LINE)
GRID = (PLANE, LINE, PAIR)
LEAD, TOOK, WIRE, SLACK = 14, 24.0, 25.0, 99
STATES, HID1, HID0 = 3.6, 4.4, 3.9
DIRECT, PACE = 0.5, 0.5
SHARES = ((3, 4, 4), (3, 3, 3, 2)), (2, 3, 3, 3)


def nn(a, b):
    return jnp.dot(a, b, preferred_element_type=F32)


def tn(a, b):
    return lax.dot_general(a, b, (((0,), (0,)), ((), ())), preferred_element_type=F32)


def nt(a, b):
    return lax.dot_general(a, b, (((1,), (1,)), ((), ())), preferred_element_type=F32)


def norm_scale(wide):
    return lax.rsqrt(jnp.mean(wide * wide, -1, keepdims=True) + 1e-6)


def norm_rows(h):
    wide = h.astype(F32)
    return (wide * norm_scale(wide)).astype(BF16)


def norm_back(da, h):
    wide, da = h.astype(F32), da.astype(F32)
    scale = norm_scale(wide)
    return (da * scale - wide * (scale * scale * scale * jnp.mean(da * wide, -1, keepdims=True))).astype(BF16)


def silu_back(gate, up, by_act):
    s = jax.nn.sigmoid(gate)
    return (by_act * up * s * (1 + gate * (1 - s))).astype(BF16), (by_act * gate * s).astype(BF16)


class Place:
    def __init__(self):
        d = lax.axis_index("dp")
        self.c, chip = d % PAIR, d // PAIR
        self.z, self.own = chip % LINE, chip // LINE
        x, y = self.own // PAIR, self.own % PAIR
        self.xs, self.ys, self.diag = (1 - x) * PAIR + y, x * PAIR + 1 - y, (1 - x) * PAIR + 1 - y
        self.near, self.far = pl.ds(self.z // PAIR * PAIR, PAIR), pl.ds(PAIR - self.z // PAIR * PAIR, PAIR)
        self.inner = jnp.logical_or(self.z == 1, self.z == 2)
        self.outer = jnp.logical_not(self.inner)
        at = lambda plane, z, c: {"dp": (plane * LINE + z) * PAIR + c}
        self.to_x, self.to_y, self.to_diag = (at(plane, self.z, self.c) for plane in (self.xs, self.ys, self.diag))
        self.to_c = at(self.own, self.z, 1 - self.c)
        self.to_z = [at(self.own, (self.z + k) % LINE, self.c) for k in range(1, LINE)]
        self.next_z = at(self.own, self.z + 1 - PAIR * (self.z % PAIR), self.c)
        self.across_z = at(self.own, LINE - 1 - self.z, self.c)
        self.sharers = [self.to_x, self.to_y, self.to_c, *self.to_z]


def signal_all(sem, devices):
    for device in devices:
        pl.semaphore_signal(sem, inc=1, device_id=device, device_id_type=MESH)


def greet(devices):
    barrier = pltpu.get_barrier_semaphore()
    signal_all(barrier, devices)
    return lambda: pl.semaphore_wait(barrier, len(devices))


def send(src, dst, send_sem, recv_sem, device):
    pltpu.make_async_remote_copy(src, dst, send_sem, recv_sem, device_id=device, device_id_type=MESH).start()


def await_bytes(ref, sem):
    pltpu.make_async_copy(ref, ref, sem).wait()


class Gather:
    Z, Z2, Z3, XA, XB, YA, YB, DX, DY, C, OWN, SENT = SLOTS = range(12)

    def __init__(self, place, mine, blocks, amount, sems, direct):
        self.p, self.mine, self.blocks, self.amount, self.sems, self.direct = place, mine, blocks, amount, sems, direct

    def z_first(self):
        p = self.p
        (here,) = self.blocks(p.own, p.z, p.c)
        pltpu.make_async_copy(self.mine, here, self.sems.at[self.OWN]).start()
        for device in p.to_z if self.direct else [p.next_z]:
            send(self.mine, here, self.sems.at[self.SENT], self.sems.at[self.Z], device)

    def _move(self, plane, zs, slot, device):
        for ref in self.blocks(plane, zs, self.p.c):
            send(ref, ref, self.sems.at[self.SENT], self.sems.at[slot], device)

    def _wait(self, slot, blocks=PAIR):
        await_bytes(self.amount(blocks), self.sems.at[slot])

    def z_second(self):
        @pl.when(self.p.inner)
        def _():
            self._wait(self.Z, 1)
            self._wait(self.OWN, 1)
            self._move(self.p.own, self.p.near, self.Z2, self.p.across_z)

    def z_third(self):
        @pl.when(self.p.inner)
        def _():
            self._wait(self.Z2)
            self._move(self.p.own, self.p.far, self.Z3, self.p.next_z)

    def plane(self):
        p = self.p
        if self.direct:
            self._wait(self.Z, LINE - 1)
            self._wait(self.OWN, 1)
        else:

            @pl.when(p.outer)
            def _():
                self._wait(self.Z, 1)
                self._wait(self.OWN, 1)
                self._wait(self.Z3)

        self._move(p.own, LO, self.XA, p.to_x)
        self._move(p.own, HI, self.YB, p.to_y)
        self._move(p.own, HI, self.XB, p.to_x)
        self._move(p.own, LO, self.YA, p.to_y)
        self._move(p.own, ALL, self.C, p.to_c)

    def across(self):
        p = self.p
        self._wait(self.XA)
        self._move(p.xs, LO, self.DY, p.to_y)
        self._wait(self.YB)
        self._move(p.ys, HI, self.DX, p.to_x)

    def to_core(self):
        p = self.p
        self._wait(self.XB)
        self._move(p.xs, ALL, self.C, p.to_c)
        self._wait(self.YA)
        self._move(p.ys, ALL, self.C, p.to_c)

    def last_to_core(self):
        self._wait(self.DY)
        self._wait(self.DX)
        self._move(self.p.diag, ALL, self.C, self.p.to_c)

    def done(self):
        self._wait(self.C, PLANE * LINE)

    def sent(self):
        for _ in range(LINE - 1 if self.direct else 1):
            await_bytes(self.mine, self.sems.at[self.SENT])
        if not self.direct:
            pl.when(self.p.inner)(functools.partial(self._wait, self.SENT, LINE))
        for _ in range(7):
            self._wait(self.SENT, LINE)


def add_into(dst, *srcs):
    def one(i, _):
        for z in range(dst.shape[1]):
            total = srcs[0][i, z].astype(F32)
            for s in srcs[1:]:
                total += s[i, z].astype(F32)
            dst[i, z] = total.astype(dst.dtype)
        return 0

    if dst.shape[0] == 1:
        one(0, 0)
    else:
        lax.fori_loop(0, dst.shape[0], one, 0)


class Scatter:
    P1X, P1Y, XA, XB, YA, YB, Z, SENT, *C, L0, L1, L2, L3 = SLOTS = range(16)
    L = (L0, L1, L2, L3)

    @staticmethod
    def scratch(n, r, w):
        return [pltpu.VMEM(s + (r, w), BF16) for s in ((PLANE, n, LINE), (PLANE, n, LINE), (n, 3 * LINE), (LINE - 1, n))]

    def __init__(self, place, n, terms, out, slot, sems, acc):
        self.p, self.n, self.terms, self.out, self.sems, self.acc = place, n, terms, out, sems, acc
        mine, other, arrived, rz = slot
        some = pl.ds(0, n)
        self.mine, self.other = (lambda g, zs=ALL: mine.at[g, some, zs]), (lambda g, zs=ALL: other.at[g, some, zs])
        self.p1x, self.p1y = arrived.at[some, LO], arrived.at[some, HI]
        self.rx, self.ry = (lambda lo: arrived.at[some, pl.ds(LINE + lo, PAIR)]), (lambda lo: arrived.at[some, pl.ds(PAIR * LINE + lo, PAIR)])
        self.rz, self.kept = rz.at[:, some], mine

    def start(self):
        p = self.p
        for g, plane in enumerate((p.diag, p.xs, p.ys, p.own)):
            for ref, part in self.terms(plane, 1 - p.c):
                send(ref, part(self.other(g)), self.sems.at[self.SENT], self.sems.at[self.C[g]], p.to_c)
            for ref, part in self.terms(plane, p.c):
                pltpu.make_async_copy(ref, part(self.mine(g)), self.sems.at[self.L[g]]).start()

    def _both(self, g):
        await_bytes(self.other(g), self.sems.at[self.C[g]])
        await_bytes(self.mine(g), self.sems.at[self.L[g]])

    def _send(self, src, dst, slot, device):
        send(src, dst, self.sems.at[self.SENT], self.sems.at[slot], device)

    def diagonal(self):
        p = self.p
        self._both(0)
        add_into(self.mine(0), self.mine(0), self.other(0))
        self._send(self.mine(0, LO), self.p1x, self.P1X, p.to_x)
        self._send(self.mine(0, HI), self.p1y, self.P1Y, p.to_y)

    def straight(self):
        p = self.p
        self._both(1)
        add_into(self.mine(1, LO), self.mine(1, LO), self.other(1, LO))
        self._send(self.mine(1, LO), self.rx(0), self.XA, p.to_x)
        self._both(2)
        add_into(self.mine(2, HI), self.mine(2, HI), self.other(2, HI))
        self._send(self.mine(2, HI), self.ry(PAIR), self.YB, p.to_y)

    def joined(self):
        p = self.p
        await_bytes(self.p1y, self.sems.at[self.P1Y])
        add_into(self.mine(1, HI), self.mine(1, HI), self.other(1, HI), self.p1y)
        self._send(self.mine(1, HI), self.rx(PAIR), self.XB, p.to_x)
        await_bytes(self.p1x, self.sems.at[self.P1X])
        add_into(self.mine(2, LO), self.mine(2, LO), self.other(2, LO), self.p1x)
        self._send(self.mine(2, LO), self.ry(0), self.YA, p.to_y)

    def along_z(self):
        p = self.p
        self._both(3)
        for part, lo, xs, ys in ((LO, 0, self.XA, self.YA), (HI, PAIR, self.XB, self.YB)):
            await_bytes(self.rx(lo), self.sems.at[xs])
            await_bytes(self.ry(lo), self.sems.at[ys])
            add_into(self.mine(3, part), self.mine(3, part), self.other(3, part), self.rx(lo), self.ry(lo))
        for k, device in enumerate(p.to_z):
            self._send(self.mine(3, (p.z + 1 + k) % LINE), self.rz.at[k], self.Z, device)

    def last(self):
        await_bytes(self.rz, self.sems.at[self.Z])
        for i in range(self.n):
            total = self.kept[3, i, self.p.z].astype(F32)
            for k in range(LINE - 1):
                total += self.rz[k, i].astype(F32)
            g = total.astype(BF16)
            self.out(i)[:] = g
            g = g.astype(F32)
            g = g * g
            r, w = g.shape
            lanes = g[:, :LANES]
            for k in range(1, w // LANES):
                lanes += g[:, LANES * k : LANES * (k + 1)]
            self.acc[:] += jnp.sum(lanes.reshape(-1, *self.acc.shape), 0)

    def sent(self):
        for _ in range(7):
            await_bytes(self.other(0), self.sems.at[self.SENT])
        await_bytes(self.rz, self.sems.at[self.SENT])


class Pump:
    def __init__(self):
        self.items, self.now = [], 0.0

    def insert(self, when, act, tag=None):
        at = len(self.items)
        while at and self.items[at - 1][0] > when:
            at -= 1
        self.items.insert(at, (when, act, tag))

    def due(self):
        acts = []
        while self.items and self.items[0][0] <= self.now:
            acts.append(self.items.pop(0)[1])
        return acts

    def through(self, tag):
        acts = []
        while any(t == tag for _, _, t in self.items):
            when, act, _ = self.items.pop(0)
            self.now = max(self.now, when)
            acts.append(act)
        return acts

    def plan(self, steps, cost, gates=None, inject=None):
        ticks = {}
        for s in range(steps):
            self.now += cost
            if inject and s in inject:
                for put in inject[s]:
                    put()
            acts = self.due()
            if gates and s + 1 in gates:
                acts += self.through(gates[s + 1])
            if acts:
                ticks[s] = acts
        return ticks


def run(acts):
    for act in acts:
        act()


def stream(steps, ins, outs, body, ticks, late=(), before=None):
    def fetch(step):
        for where, buf, sem in ins:
            pltpu.make_async_copy(where(step), buf.at[step % PAIR], sem.at[step % PAIR]).start()

    def one(step, _):
        slot = step % PAIR
        early = step + 1 < steps
        for t in late:
            early = jnp.logical_and(early, step != t)
        pl.when(early)(lambda: fetch(step + 1))
        for _, buf, sem in ins:
            await_bytes(buf.at[slot], sem.at[slot])
        body(step, [buf.at[slot] for _, buf, _ in ins], [buf.at[slot] for _, buf, _ in outs])

        @pl.when(step >= 1)
        def _():
            for _, buf, sem in outs:
                await_bytes(buf.at[1 - slot], sem.at[1 - slot])

        for where, buf, sem in outs:
            pltpu.make_async_copy(buf.at[slot], where(step), sem.at[slot]).start()
        for t, acts in plan.items():
            pl.when(step == t)(functools.partial(run, acts))
        for t in late:
            pl.when(step == t)(lambda t=t: fetch(t + 1))
        return 0

    fetch(0)
    if before is not None:
        before()
    plan = ticks()
    lax.fori_loop(0, steps, one, 0)
    for _, buf, sem in outs:
        await_bytes(buf.at[(steps - 1) % PAIR], sem.at[(steps - 1) % PAIR])


def cols(step, width):
    return pl.ds(pl.multiple_of(step * width, width), width)


def cuts(total, *shares):
    whole, at, parts = sum(shares), 0, []
    for k in range(len(shares)):
        end = -(-total * sum(shares[: k + 1]) // whole)
        if end > at:
            parts.append((at, end - at))
        at = end
    return parts


def concat(ref, n):
    return jnp.concatenate([ref[j] for j in range(n)], axis=-1)


shape = jax.ShapeDtypeStruct
any_, whole = pl.BlockSpec(memory_space=pl.ANY), pl.BlockSpec(memory_space=pltpu.VMEM)


def two(*dims, dtype=BF16):
    return pltpu.VMEM((PAIR, *dims), dtype)


class Sizes:
    def __init__(self, tokens, d, ff):
        self.tokens, self.d, self.ff, self.half = tokens, d, ff, d // PAIR
        self.tiles, self.rd, self.rf = ff // TILE, d // DEVICES, ff // DEVICES
        self.parts = cuts(self.tiles, *SHARES[1])
        self.deep, self.tall, self.wide = (self.tiles, *GRID, self.rd, TILE), (ff, d), (self.tiles, tokens, TILE)
        self.thin, self.turned = (tokens, d), (d, tokens)
        self.blocks = [shape((self.rd, ff), BF16)] * PAIR + [shape((self.rf, d), BF16)]
        slots = Scatter.scratch(1, self.rf, self.half) * PAIR
        for _, size in self.parts:
            slots += Scatter.scratch(size, self.rd, TILE) * PAIR
        self.n_slots = PAIR + PAIR * len(self.parts)
        self.slot_size, self.slots = len(slots) // self.n_slots, slots
        many = PAIR if tokens % (PAIR * LINE * TILE) == 0 else 1
        self.halves = [pl.ds(q * (tokens // many), tokens // many) for q in range(many)]
        self.hidden_bufs = [two(tokens, TILE, dtype=F32)] * PAIR + [two(TILE, d)] + [two(tokens, TILE)] * PAIR
        self.hidden_bufs += [two(*GRID, self.rd, TILE)] * PAIR + [two(TILE, d)]


def block_rows(plane, z, c, r):
    return pl.ds(pl.multiple_of(((plane * LINE + z) * PAIR + c) * r, 8), r)


def piece(refs, bufs, sems):
    return [(lambda s, ref=ref: ref.at[s], buf, sems.at[k]) for k, (ref, buf) in enumerate(zip(refs, bufs))]


def scatters(place, pump, size, slots, sems, acc, out, down, wide):
    state = {"free": 0.0}

    def scatter(n, terms, to, slot, share):
        one = Scatter(place, n, terms, to, slots[slot], sems.at[slot], acc)
        wire = WIRE * share

        def put():
            now = pump.now
            start = max(now + 3, min(state["free"], now + SLACK * wire))
            state["free"] = start + wire
            ahead, end = max(now + 3, start - 4), start + 1.6 * wire + 5
            acts = [(now, one.start), (ahead, one.diagonal), (ahead, one.straight), (start + 0.4 * wire, one.joined)]
            acts += [(start + wire + 2, one.along_z), (end, one.last), (end, one.sent)]
            for when, act in acts:
                pump.insert(when, act)

        return put

    def down_job(k):
        part = pl.ds(k * size.half, size.half)
        terms = lambda plane, c: [(down.at[block_rows(plane, z, c, size.rf), part], lambda to, z=z: to.at[0, z]) for z in range(LINE)]
        return scatter(1, terms, lambda i: out[-1].at[:, part], k, 0.5)

    def wide_job(b, k):
        start, n = size.parts[b]
        terms = lambda plane, c: [(wide[k].at[pl.ds(start, n), plane, :, c], lambda to: to)]
        to = lambda i: out[k].at[:, pl.ds((start + i) * TILE, TILE)]
        return scatter(n, terms, to, PAIR + PAIR * b + k, n / size.tiles)

    jobs = [[down_job(k) for k in range(PAIR)]] + [[wide_job(b, k) for k in range(PAIR)] for b in range(len(size.parts))]

    def put_all(puts):
        for put in puts:
            put()

    return [functools.partial(put_all, puts) for puts in jobs]


def hidden(size, pump, by, at, ins, grads, kept, puts, cost, before, sems, gbuf, ubuf, wdbuf, dgbuf, dubuf, gout, uout, wbuf):
    in_sem, out_sem = sems
    gate, up, w_down = ins

    def body(step, ins, outs):
        dg, du = outs[PAIR:] if kept else (dgbuf.at[0], dubuf.at[0])
        for part in size.halves:
            by_act = nt(by[part, :], ins[2][:]).astype(BF16).astype(F32)
            dg[part, :], du[part, :] = silu_back(ins[0][part, :], ins[1][part, :], by_act)
        for out, grad in zip(outs, (dg, du)):
            out[:] = nn(at[:], grad[:]).astype(BF16).reshape(*GRID, size.rd, TILE)

    outs = piece((*grads, *kept), (gout, uout, dgbuf, dubuf)[: PAIR + len(kept)], out_sem)
    inject = {min(start + n, size.tiles - 1): [put] for (start, n), put in zip(size.parts, puts[:-1])}
    streams = piece((gate, up), (gbuf, ubuf), in_sem)
    streams.append((lambda s: w_down.at[cols(s, TILE), :], wdbuf, in_sem.at[2]))
    before = before and functools.partial(before, dgbuf, wbuf)
    stream(size.tiles, streams, outs, body, lambda: pump.plan(size.tiles, cost, inject=inject), before=before)
    puts[-1]()
    run(pump.due())


def first_part(x, dy, weights):
    size = Sizes(*x.shape, weights[0].shape[-1])
    tokens, d, ff, tiles, rd, rf, half = size.tokens, size.d, size.ff, size.tiles, size.rd, size.rf, size.half
    rows, few = tokens // LINE, tokens // (PAIR * LINE)
    chunks = [cuts(tiles, *shares) for shares in SHARES[0]]
    jobs_of, gates = [], [{}, {}]
    for layer in range(PAIR):
        for start, n in chunks[layer]:
            if layer and start == chunks[1][-1][0]:
                jobs_of.append((1, 2, 0, half))
            jobs_of += [(layer, 0, start, n), (layer, 1, start, n)]
            gates[layer][start] = len(jobs_of) - 1
        jobs_of += [(1, 2, half, half)] if layer else [(0, 2, 0, half), (0, 2, half, half)]
        gates[layer]["down"] = len(jobs_of) - 1
    nj = len(jobs_of)
    held_shapes = [(PAIR, tiles, rd, TILE), (PAIR, tiles, rd, TILE), (PAIR, rf, d)]
    deep, tall, wide, thin, turned = size.deep, size.tall, size.wide, size.thin, size.turned
    hbm = [turned, wide, deep, deep, tall, deep, deep, tall, thin, tall, wide, wide, deep, deep]
    hbm = [shape(thin, BF16), shape(tall, BF16), shape(wide, F32), shape(wide, F32)] + [shape(dims, BF16) for dims in hbm]
    hbm += [shape(wide, F32)] * PAIR
    scratch = [pltpu.VMEM(dims, BF16) for dims in held_shapes + [thin, thin, turned, deep]]

    def kernel(*refs):
        it = iter(refs)
        take = lambda n: [next(it) for _ in range(n)]
        x_hbm, dy_hbm, *w_hbm = take(PAIR + len(weights))
        *out, acc = take(len(weights) + 1)
        dh1, dwd0, gate0, up0, a0t, act0, g0, u0, d0, g1, u1, d1, h1_hbm, dwd1, dg1, du1, dwg1, dwu1, gate1, up1 = take(len(hbm))
        full = [[g0, u0, d0], [g1, u1, d1]]
        *held, a, by, at, wg = take(len(scratch))
        slots = [take(size.slot_size) for _ in range(size.n_slots)]
        load_sem, ag_sems, rs_sems, in_sem, out_sem, one_sem = take(6)
        s_x, s_at, s_w, s_u = (one_sem.at[k] for k in range(4))
        place = Place()

        def load(k, layer):
            ref, sem = w_hbm[k].at[layer], load_sem.at[k, layer]
            if k == PAIR:
                pltpu.make_async_copy(ref, held[k].at[layer], sem).start()
            else:
                for t in range(tiles):
                    pltpu.make_async_copy(ref.at[:, pl.ds(TILE * t, TILE)], held[k].at[layer, t], sem).start()

        x_load = pltpu.make_async_copy(x_hbm, by, s_x)
        greeting = greet(place.sharers)
        for layer in range(PAIR):
            for k in range(len(held)):
                load(k, layer)
                if k == 1 and not layer:
                    x_load.start()
        greeting()
        acc[:] = jnp.zeros_like(acc)
        pump, jobs, loaded = Pump(), [], set()

        def first(j):
            layer, k, _, _ = jobs_of[j]
            if (k, layer) not in loaded:
                await_bytes(held[k].at[layer], load_sem.at[k, layer])
                loaded.add((k, layer))
            jobs[j].z_first()

        clock = begun = 4.0
        for j, (layer, k, start, n) in enumerate(jobs_of):
            part, ref = pl.ds(start, n), full[layer][k]
            if k == PAIR:

                def blocks(plane, zs, c, ref=ref, part=part):
                    zs = [zs.start + i for i in range(zs.size)] if isinstance(zs, pl.Slice) else [zs]
                    return [ref.at[block_rows(plane, z, c, rf), part] for z in zs]

                amount = lambda n, ref=ref, part=part: ref.at[pl.ds(0, n * rf), part]
                mine = held[k].at[layer, :, part]
            else:
                blocks = lambda plane, zs, c, ref=ref, part=part: [ref.at[part, plane, zs, c]]
                amount = lambda n, ref=ref, part=part: ref.at[part, pl.ds(0, max(1, n // LINE)), pl.ds(0, min(n, LINE)), 0]
                mine = held[k].at[layer, part]
            job = Gather(place, mine, blocks, amount, ag_sems.at[j], j < PAIR)
            jobs.append(job)
            took = TOOK * n / (d if k == PAIR else tiles)
            unit = took / 6
            lead = min(max(0.33 * clock - 5, 3), LEAD)
            zero = begun - 4
            pump.insert(zero, functools.partial(first, j))
            if not job.direct:
                pump.insert(zero + unit + 2.5, job.z_second)
                pump.insert(zero + 3 * unit + 5, job.z_third)
            ready = max(zero + 5 * unit + (5 if job.direct else 7.5), clock - lead)
            clock = max(clock, ready)
            pump.insert(ready, job.plane)
            pump.insert(clock + 0.4 * took, job.across)
            pump.insert(clock + 0.75 * took, job.to_core)
            behind = PAIR if j >= nj - 3 else lead
            pump.insert(clock + took + behind + 1, job.last_to_core)
            pump.insert(clock + took + behind + 2, job.done, j)
            clock += took
            begun += (PACE if j > 1 else DIRECT) * took
        pump.now = 3.0
        run(pump.due())
        x_load.wait()
        a0_out = pltpu.make_async_copy(at, a0t, s_at)
        dy_load = pltpu.make_async_copy(dy_hbm, by, s_x)

        step = min(TILE, tokens)

        def norm(i, _):
            part = cols(i, step)
            normed = norm_rows(by[part, :])
            a[part, :] = normed
            at[:, part] = normed.T
            return 0

        lax.fori_loop(0, tokens // step, norm, 0)
        a0_out.start()
        pump.now = 8.0

        def gate_up(layer, gate, up, before, wgate, wup, gbuf, ubuf, actbuf, dwbuf):
            def body(step, ins, outs):
                g = nn(a[:], ins[0][:].reshape(d, TILE))
                u = nn(a[:], ins[1][:].reshape(d, TILE))
                outs[0][:] = g
                outs[1][:] = u
                product = (g * jax.nn.sigmoid(g) * u).astype(BF16)
                if layer:
                    actbuf[0] = product
                    outs[2][:] = tn(actbuf[0], by[:]).astype(BF16)
                else:
                    outs[2][:] = product

            run(pump.through(gates[layer][0]))
            later = {s: j for s, j in gates[layer].items() if s in range(1, tiles)}
            outs = piece((gate, up, act0), (gbuf, ubuf, actbuf), out_sem)
            if layer:
                outs[-1] = (lambda s: dwd1.at[cols(s, TILE), :], dwbuf, out_sem.at[2])
            stream(
                tiles,
                piece(full[layer][:PAIR], (wgate, wup), in_sem),
                outs,
                body,
                lambda: pump.plan(tiles, 3.7 if layer else 2.5, later),
                late=[s - 1 for s in later],
                before=before,
            )

        def down(wd, tall, hbuf):
            run(pump.through(gates[0]["down"]))
            wd_load = pltpu.make_async_copy(d0, wd, s_w)
            wd_load.start()

            def ready():
                a0_out.wait()
                wd_load.wait()

            def body(step, ins, outs):
                part = cols(step, rows)
                h = by[part, :] + nn(concat(ins[0], tiles), wd[:]).astype(BF16)
                outs[0][:] = h
                normed = norm_rows(h)
                a[part, :] = normed
                at[:, part] = normed.T

            stream(
                tokens // rows,
                [(lambda s: act0.at[:, cols(s, rows), :], tall, in_sem.at[0])],
                [(lambda s: h1_hbm.at[cols(s, rows), :], hbuf, out_sem.at[0])],
                body,
                lambda: pump.plan(tokens // rows, 3.8),
                before=ready,
            )
            dy_load.start()

        tile_bufs = [two(*GRID, rd, TILE)] * PAIR + [two(tokens, TILE, dtype=F32)] * PAIR + [two(tokens, TILE), two(TILE, d)]
        pl.run_scoped(functools.partial(gate_up, 0, gate0, up0, None), *tile_bufs)
        pl.run_scoped(down, pltpu.VMEM(d0.shape, BF16), two(tiles, rows, TILE), two(rows, d))
        pl.run_scoped(functools.partial(gate_up, 1, gate1, up1, dy_load.wait), *tile_bufs)
        run(pump.through(nj - 1))
        assert not pump.items
        put_down, *put_wide = scatters(place, pump, size, slots, rs_sems, acc, out, dwd1, (dwg1, dwu1))
        put_down()
        run(pump.due())
        wg_load = pltpu.make_async_copy(g1, wg, s_w)
        wg_load.start()
        ins, grads = (gate1, up1, d1), (dwg1, dwu1)
        pl.run_scoped(
            functools.partial(hidden, size, pump, by, at, ins, grads, (dg1, du1), put_wide, HID1, None, (in_sem, out_sem)), *size.hidden_bufs
        )

        def states(wu, dgbuf, dubuf, hbuf):
            wu_load = pltpu.make_async_copy(u1, wu, s_u)
            wu_load.start()

            def ready():
                wg_load.wait()
                wu_load.wait()

            def body(step, ins, outs):
                part = cols(step, few)
                dg, du, h = (ref for ref in ins)
                da = nt(concat(dg, tiles), concat(wg, tiles).reshape(d, ff)) + nt(concat(du, tiles), concat(wu, tiles).reshape(d, ff))
                by[part, :] = by[part, :] + norm_back(da.astype(BF16), h[:])

            ins = [(lambda s, ref=ref: ref.at[:, cols(s, few), :], buf, in_sem.at[k]) for k, (ref, buf) in enumerate(((dg1, dgbuf), (du1, dubuf)))]
            ins.append((lambda s: h1_hbm.at[cols(s, few), :], hbuf, in_sem.at[2]))
            stream(tokens // few, ins, [], body, lambda: pump.plan(tokens // few, STATES), before=ready)

        pl.run_scoped(states, pltpu.VMEM(wg.shape, BF16), two(tiles, few, TILE), two(tiles, few, TILE), two(few, d))
        by_out = pltpu.make_async_copy(by, dh1, s_x)
        by_out.start()

        def down_gradient(abuf, wbuf):
            def body(step, ins, outs):
                outs[0][:] = tn(ins[0][:], by[:]).astype(BF16)

            outs = [(lambda s: dwd0.at[cols(s, TILE), :], wbuf, out_sem.at[0])]
            stream(tiles, piece((act0,), (abuf,), in_sem), outs, body, lambda: pump.plan(tiles, 1.4))

        pl.run_scoped(down_gradient, two(tokens, TILE), two(TILE, d))
        pump.now = 1e9
        run(pump.due())
        for job in jobs:
            job.sent()
        by_out.wait()

    DMA = pltpu.SemaphoreType.DMA
    outs = pl.pallas_call(
        kernel,
        name="first_part",
        in_specs=[any_] * (PAIR + len(weights)),
        out_specs=[whole] * (len(weights) + 1) + [any_] * len(hbm),
        out_shape=size.blocks + [shape((8, LANES), F32)] + hbm,
        scratch_shapes=scratch
        + size.slots
        + [DMA((3, PAIR)), DMA((nj, len(Gather.SLOTS))), DMA((size.n_slots, len(Scatter.SLOTS)))]
        + [DMA((4, PAIR)), DMA((4, PAIR)), DMA((4,))],
        compiler_params=pltpu.CompilerParams(collective_id=0, has_side_effects=True, vmem_limit_bytes=66_500_000),
    )(x, dy, *weights)
    *sums, acc = outs[: len(weights) + 1]
    dh1, dwd0, gate0, up0, a0t, _, _, _, d0 = outs[len(weights) + 1 :][:9]
    return sums, acc, (dh1, dwd0, gate0, up0, a0t, d0)


def second_part(last_acc, dh1, dwd0, gate0, up0, a0t, d0):
    size = Sizes(*dh1.shape, d0.shape[0])
    deep = shape(size.deep, BF16)
    n = len(size.blocks)

    def kernel(*refs):
        it = iter(refs)
        take = lambda n: [next(it) for _ in range(n)]
        acc_in, dh1_hbm, dwd0, gate0, up0, a0t, d0 = take(7)
        *out, squares = take(n + 1)
        dwg0, dwu0 = take(PAIR)
        by, at = take(PAIR)
        slots = [take(size.slot_size) for _ in range(size.n_slots)]
        acc, sums, gone, rs_sems, in_sem, out_sem, sums_sem, one_sem = take(8)
        place, pump = Place(), Pump()
        by_load, at_load = pltpu.make_async_copy(dh1_hbm, by, one_sem.at[0]), pltpu.make_async_copy(a0t, at, one_sem.at[1])
        by_load.start()
        at_load.start()
        greeting = greet(place.sharers + [place.to_diag])

        def ready(*_):
            greeting()
            put_down()
            run(pump.due())
            acc[:] = acc_in[:]
            by_load.wait()
            at_load.wait()

        put_down, *put_wide = scatters(place, pump, size, slots, rs_sems, acc, out, dwd0, (dwg0, dwu0))
        ins, grads = (gate0, up0, d0), (dwg0, dwu0)
        pl.run_scoped(
            functools.partial(hidden, size, pump, by, at, ins, grads, (), put_wide, HID0, ready, (in_sem, out_sem)), *size.hidden_bufs
        )
        pump.now = 1e9
        run(pump.due())
        sums[0] = jnp.full(acc.shape, jnp.sum(acc[:]), F32)
        hops = [[place.to_c], [place.to_x, place.to_y, place.to_diag], place.to_z]
        at_gone = 0
        for k, devices in enumerate(hops):
            for i, device in enumerate(devices):
                send(sums.at[k], gone.at[at_gone + i], sums_sem.at[len(hops)], sums_sem.at[k], device)
            await_bytes(gone.at[pl.ds(at_gone, len(devices))], sums_sem.at[k])
            total = sums[k]
            for i in range(len(devices)):
                total += gone[at_gone + i]
            at_gone += len(devices)
            if k < len(hops) - 1:
                sums[k + 1] = total
            else:
                squares[:] = total
        await_bytes(gone, sums_sem.at[len(hops)])

    DMA = pltpu.SemaphoreType.DMA
    tile = (8, LANES)
    *sums, squares = pl.pallas_call(
        kernel,
        name="second_part",
        in_specs=[whole] + [any_] * 6,
        out_specs=[whole] * (n + 1) + [any_] * PAIR,
        out_shape=size.blocks + [shape(tile, F32)] + [deep, deep],
        scratch_shapes=[pltpu.VMEM(size.thin, BF16), pltpu.VMEM(size.turned, BF16)]
        + size.slots
        + [pltpu.VMEM(tile, F32), pltpu.VMEM((3, *tile), F32), pltpu.VMEM((7, *tile), F32)]
        + [DMA((size.n_slots, len(Scatter.SLOTS))), DMA((4, PAIR)), DMA((4, PAIR)), DMA((4,)), DMA((PAIR,))],
        compiler_params=pltpu.CompilerParams(collective_id=1, has_side_effects=True, vmem_limit_bytes=66_500_000),
    )(last_acc, dh1, dwd0, gate0, up0, a0t, d0)[: n + 1]
    return sums, squares


def adamw(weights, m, v, sums, squares):
    n = len(weights)
    count = DEVICES * sum(w.size for w in weights)

    def kernel(squares_ref, *refs):
        factor = jnp.minimum(1.0, 0.5 * lax.rsqrt(squares_ref[:1, :1] / count + 1e-30))
        for k in range(n):
            w, m, v, g, last_g, new_w, new_m, new_v = refs[k::n]
            grad = jnp.where(pl.program_id(0) == 0, g[:].astype(F32), last_g[:].astype(F32)) * factor
            m_next = 0.9 * m[0] + 0.1 * grad
            v_next = 0.95 * v[0] + 0.05 * grad * grad
            wide = w[0].astype(F32)
            new_w[0] = (wide - 0.02 * (m_next * lax.rsqrt(v_next + 1e-8) + 0.1 * wide)).astype(BF16)
            new_m[0] = m_next
            new_v[0] = v_next

    blocks = [pl.BlockSpec((1, *w.shape[1:]), lambda layer: (layer, 0, 0)) for w in weights]
    once = [pl.BlockSpec(s.shape, lambda layer: (0, 0)) for s in (squares, *sums)]
    return pl.pallas_call(
        kernel,
        name="adamw",
        grid=(PAIR,),
        in_specs=once[:1] + blocks * 3 + once[1:],
        out_specs=blocks * 3,
        out_shape=[shape(w.shape, BF16) for w in weights] + [shape(w.shape, F32) for w in weights] * PAIR,
    )(squares, *weights, *m, *v, *sums)


def solution(mesh):
    def step(x, dy, *arrays):
        weights, m, v = (arrays[3 * i : 3 * i + 3] for i in range(3))
        last, acc, kept = first_part(x[0], dy[0], weights)
        sums, squares = second_part(acc, *kept)
        return tuple(adamw(weights, m, v, [*sums, *last], squares))

    states, cut = P(("rep", "dp"), None, None), P(None, "dp", None)
    return jax.shard_map(
        step,
        mesh=mesh,
        in_specs=(states, states) + (cut,) * 9,
        out_specs=(P("rep", "dp", None),) * 9,
        check_vma=False,
    )
```

```python
import functools

import jax
import jax.numpy as jnp
from jax import lax
from jax.experimental import pallas as pl
from jax.experimental.pallas import tpu as pltpu
from jax.sharding import PartitionSpec as P

F32, BF16 = jnp.float32, jnp.bfloat16
MESH = pl.DeviceIdType.MESH
DEVICES, PLANE, LINE, TILE, LANES = 32, 4, 4, 256, 128
PAIR = 2
LO, HI, ALL = pl.ds(0, PAIR), pl.ds(PAIR, PAIR), pl.ds(0, LINE)
GRID = (PLANE, LINE, PAIR)
LEAD, TOOK = 14, 24.0
TEMPOS = (25.0, 4, 1.6), (25.0, 6, 1.6)
STATES, HID1, HID0 = 3.6, 4.4, 3.9
DIRECT, PACE = 0.5, 0.5
SHARES = ((3, 4, 4), (3, 3, 3, 2)), (3, 3, 3, 2), (2, 3, 3, 3)


def nn(a, b):
    return jnp.dot(a, b, preferred_element_type=F32)


def tn(a, b):
    return lax.dot_general(a, b, (((0,), (0,)), ((), ())), preferred_element_type=F32)


def nt(a, b):
    return lax.dot_general(a, b, (((1,), (1,)), ((), ())), preferred_element_type=F32)


def norm_scale(wide):
    return lax.rsqrt(jnp.mean(wide * wide, -1, keepdims=True) + 1e-6)


def norm_rows(h):
    wide = h.astype(F32)
    return (wide * norm_scale(wide)).astype(BF16)


def norm_back(da, h):
    wide, da = h.astype(F32), da.astype(F32)
    scale = norm_scale(wide)
    return (da * scale - wide * (scale * scale * scale * jnp.mean(da * wide, -1, keepdims=True))).astype(BF16)


def silu_back(gate, up, by_act):
    s = jax.nn.sigmoid(gate)
    return (by_act * up * s * (1 + gate * (1 - s))).astype(BF16), (by_act * gate * s).astype(BF16)


class Place:
    def __init__(self):
        d = lax.axis_index("dp")
        self.c, chip = d % PAIR, d // PAIR
        self.z, self.own = chip % LINE, chip // LINE
        x, y = self.own // PAIR, self.own % PAIR
        self.xs, self.ys, self.diag = (1 - x) * PAIR + y, x * PAIR + 1 - y, (1 - x) * PAIR + 1 - y
        self.near, self.far = pl.ds(self.z // PAIR * PAIR, PAIR), pl.ds(PAIR - self.z // PAIR * PAIR, PAIR)
        self.inner = jnp.logical_or(self.z == 1, self.z == 2)
        self.outer = jnp.logical_not(self.inner)
        at = lambda plane, z, c: {"dp": (plane * LINE + z) * PAIR + c}
        self.to_x, self.to_y, self.to_diag = (at(plane, self.z, self.c) for plane in (self.xs, self.ys, self.diag))
        self.to_c = at(self.own, self.z, 1 - self.c)
        self.to_z = [at(self.own, (self.z + k) % LINE, self.c) for k in range(1, LINE)]
        self.next_z = at(self.own, self.z + 1 - PAIR * (self.z % PAIR), self.c)
        self.across_z = at(self.own, LINE - 1 - self.z, self.c)
        self.sharers = [self.to_x, self.to_y, self.to_c, *self.to_z]


def signal_all(sem, devices):
    for device in devices:
        pl.semaphore_signal(sem, inc=1, device_id=device, device_id_type=MESH)


def greet(devices):
    barrier = pltpu.get_barrier_semaphore()
    signal_all(barrier, devices)
    return lambda: pl.semaphore_wait(barrier, len(devices))


def send(src, dst, send_sem, recv_sem, device):
    pltpu.make_async_remote_copy(src, dst, send_sem, recv_sem, device_id=device, device_id_type=MESH).start()


def await_bytes(ref, sem):
    pltpu.make_async_copy(ref, ref, sem).wait()


class Gather:
    Z, Z2, Z3, XA, XB, YA, YB, DX, DY, C, OWN, SENT = SLOTS = range(12)

    def __init__(self, place, mine, blocks, amount, sems, direct):
        self.p, self.mine, self.blocks, self.amount, self.sems, self.direct = place, mine, blocks, amount, sems, direct

    def z_first(self):
        p = self.p
        (here,) = self.blocks(p.own, p.z, p.c)
        pltpu.make_async_copy(self.mine, here, self.sems.at[self.OWN]).start()
        for device in p.to_z if self.direct else [p.next_z]:
            send(self.mine, here, self.sems.at[self.SENT], self.sems.at[self.Z], device)

    def _move(self, plane, zs, slot, device):
        for ref in self.blocks(plane, zs, self.p.c):
            send(ref, ref, self.sems.at[self.SENT], self.sems.at[slot], device)

    def _wait(self, slot, blocks=PAIR):
        await_bytes(self.amount(blocks), self.sems.at[slot])

    def z_second(self):
        @pl.when(self.p.inner)
        def _():
            self._wait(self.Z, 1)
            self._wait(self.OWN, 1)
            self._move(self.p.own, self.p.near, self.Z2, self.p.across_z)

    def z_third(self):
        @pl.when(self.p.inner)
        def _():
            self._wait(self.Z2)
            self._move(self.p.own, self.p.far, self.Z3, self.p.next_z)

    def plane(self):
        p = self.p
        if self.direct:
            self._wait(self.Z, LINE - 1)
            self._wait(self.OWN, 1)
        else:

            @pl.when(p.outer)
            def _():
                self._wait(self.Z, 1)
                self._wait(self.OWN, 1)
                self._wait(self.Z3)

        self._move(p.own, LO, self.XA, p.to_x)
        self._move(p.own, HI, self.YB, p.to_y)
        self._move(p.own, HI, self.XB, p.to_x)
        self._move(p.own, LO, self.YA, p.to_y)
        self._move(p.own, ALL, self.C, p.to_c)

    def across(self):
        p = self.p
        self._wait(self.XA)
        self._move(p.xs, LO, self.DY, p.to_y)
        self._wait(self.YB)
        self._move(p.ys, HI, self.DX, p.to_x)

    def to_core(self):
        p = self.p
        self._wait(self.XB)
        self._move(p.xs, ALL, self.C, p.to_c)
        self._wait(self.YA)
        self._move(p.ys, ALL, self.C, p.to_c)

    def last_to_core(self):
        self._wait(self.DY)
        self._wait(self.DX)
        self._move(self.p.diag, ALL, self.C, self.p.to_c)

    def done(self):
        self._wait(self.C, PLANE * LINE)

    def sent(self):
        for _ in range(LINE - 1 if self.direct else 1):
            await_bytes(self.mine, self.sems.at[self.SENT])
        if not self.direct:
            pl.when(self.p.inner)(functools.partial(self._wait, self.SENT, LINE))
        for blocks in (PLANE, PLANE - 1):
            self._wait(self.SENT, blocks * LINE)


def add_into(dst, *srcs):
    def one(i, _):
        for z in range(dst.shape[1]):
            total = srcs[0][i, z].astype(F32)
            for s in srcs[1:]:
                total += s[i, z].astype(F32)
            dst[i, z] = total.astype(dst.dtype)
        return 0

    if dst.shape[0] == 1:
        one(0, 0)
    else:
        lax.fori_loop(0, dst.shape[0], one, 0)


class Scatter:
    P1X, P1Y, XA, XB, YA, YB, Z, SENT, *C, L0, L1, L2, L3 = SLOTS = range(16)
    L = (L0, L1, L2, L3)

    @staticmethod
    def scratch(n, r, w):
        return [pltpu.VMEM(s + (r, w), BF16) for s in ((PLANE, n, LINE), (PLANE, n, LINE), (n, 3 * LINE), (LINE - 1, n))]

    def __init__(self, place, n, terms, out, slot, sems, acc):
        self.p, self.n, self.terms, self.out, self.sems, self.acc = place, n, terms, out, sems, acc
        mine, other, arrived, rz = slot
        some = pl.ds(0, n)
        self.mine, self.other = (lambda g, zs=ALL: mine.at[g, some, zs]), (lambda g, zs=ALL: other.at[g, some, zs])
        self.p1x, self.p1y = arrived.at[some, LO], arrived.at[some, HI]
        self.rx, self.ry = (lambda lo: arrived.at[some, pl.ds(LINE + lo, PAIR)]), (lambda lo: arrived.at[some, pl.ds(PAIR * LINE + lo, PAIR)])
        self.rz, self.kept = rz.at[:, some], mine

    def start(self):
        p = self.p
        for g, plane in enumerate((p.diag, p.xs, p.ys, p.own)):
            for ref, part in self.terms(plane, 1 - p.c):
                send(ref, part(self.other(g)), self.sems.at[self.SENT], self.sems.at[self.C[g]], p.to_c)
            for ref, part in self.terms(plane, p.c):
                pltpu.make_async_copy(ref, part(self.mine(g)), self.sems.at[self.L[g]]).start()

    def _both(self, g):
        await_bytes(self.other(g), self.sems.at[self.C[g]])
        await_bytes(self.mine(g), self.sems.at[self.L[g]])

    def _send(self, src, dst, slot, device):
        send(src, dst, self.sems.at[self.SENT], self.sems.at[slot], device)

    def diagonal(self):
        p = self.p
        self._both(0)
        add_into(self.mine(0), self.mine(0), self.other(0))
        self._send(self.mine(0, LO), self.p1x, self.P1X, p.to_x)
        self._send(self.mine(0, HI), self.p1y, self.P1Y, p.to_y)

    def straight(self):
        p = self.p
        self._both(1)
        add_into(self.mine(1, LO), self.mine(1, LO), self.other(1, LO))
        self._send(self.mine(1, LO), self.rx(0), self.XA, p.to_x)
        self._both(2)
        add_into(self.mine(2, HI), self.mine(2, HI), self.other(2, HI))
        self._send(self.mine(2, HI), self.ry(PAIR), self.YB, p.to_y)

    def joined(self):
        p = self.p
        await_bytes(self.p1y, self.sems.at[self.P1Y])
        add_into(self.mine(1, HI), self.mine(1, HI), self.other(1, HI), self.p1y)
        self._send(self.mine(1, HI), self.rx(PAIR), self.XB, p.to_x)
        await_bytes(self.p1x, self.sems.at[self.P1X])
        add_into(self.mine(2, LO), self.mine(2, LO), self.other(2, LO), self.p1x)
        self._send(self.mine(2, LO), self.ry(0), self.YA, p.to_y)

    def along_z(self):
        p = self.p
        self._both(3)
        for part, lo, xs, ys in ((LO, 0, self.XA, self.YA), (HI, PAIR, self.XB, self.YB)):
            await_bytes(self.rx(lo), self.sems.at[xs])
            await_bytes(self.ry(lo), self.sems.at[ys])
            add_into(self.mine(3, part), self.mine(3, part), self.other(3, part), self.rx(lo), self.ry(lo))
        for k, device in enumerate(p.to_z):
            self._send(self.mine(3, (p.z + 1 + k) % LINE), self.rz.at[k], self.Z, device)

    def last(self):
        await_bytes(self.rz, self.sems.at[self.Z])
        for i in range(self.n):
            total = self.kept[3, i, self.p.z].astype(F32)
            for k in range(LINE - 1):
                total += self.rz[k, i].astype(F32)
            g = total.astype(BF16)
            self.out(i)[:] = g
            g = g.astype(F32)
            g = g * g
            r, w = g.shape
            lanes = g[:, :LANES]
            for k in range(1, w // LANES):
                lanes += g[:, LANES * k : LANES * (k + 1)]
            self.acc[:] += jnp.sum(lanes.reshape(-1, *self.acc.shape), 0)

    def sent(self):
        for _ in range(7):
            await_bytes(self.other(0), self.sems.at[self.SENT])
        await_bytes(self.rz, self.sems.at[self.SENT])


class Pump:
    def __init__(self):
        self.items, self.now = [], 0.0

    def insert(self, when, act, tag=None):
        at = len(self.items)
        while at and self.items[at - 1][0] > when:
            at -= 1
        self.items.insert(at, (when, act, tag))

    def due(self):
        acts = []
        while self.items and self.items[0][0] <= self.now:
            acts.append(self.items.pop(0)[1])
        return acts

    def through(self, tag):
        acts = []
        while any(t == tag for _, _, t in self.items):
            when, act, _ = self.items.pop(0)
            self.now = max(self.now, when)
            acts.append(act)
        return acts

    def plan(self, steps, cost, gates=None, inject=None):
        ticks = {}
        for s in range(steps):
            self.now += cost
            if inject and s in inject:
                for put in inject[s]:
                    put()
            acts = self.due()
            if gates and s + 1 in gates:
                acts += self.through(gates[s + 1])
            if acts:
                ticks[s] = acts
        return ticks


def run(acts):
    for act in acts:
        act()


def stream(steps, ins, outs, body, ticks, late=(), before=None):
    def fetch(step):
        for where, buf, sem in ins:
            pltpu.make_async_copy(where(step), buf.at[step % PAIR], sem.at[step % PAIR]).start()

    def one(step, _):
        slot = step % PAIR
        early = step + 1 < steps
        for t in late:
            early = jnp.logical_and(early, step != t)
        pl.when(early)(lambda: fetch(step + 1))
        for _, buf, sem in ins:
            await_bytes(buf.at[slot], sem.at[slot])
        body(step, [buf.at[slot] for _, buf, _ in ins], [buf.at[slot] for _, buf, _ in outs])

        @pl.when(step >= 1)
        def _():
            for _, buf, sem in outs:
                await_bytes(buf.at[1 - slot], sem.at[1 - slot])

        for where, buf, sem in outs:
            pltpu.make_async_copy(buf.at[slot], where(step), sem.at[slot]).start()
        for t, acts in plan.items():
            pl.when(step == t)(functools.partial(run, acts))
        for t in late:
            pl.when(step == t)(lambda t=t: fetch(t + 1))
        return 0

    fetch(0)
    if before is not None:
        before()
    plan = ticks()
    lax.fori_loop(0, steps, one, 0)
    for _, buf, sem in outs:
        await_bytes(buf.at[(steps - 1) % PAIR], sem.at[(steps - 1) % PAIR])


def cols(step, width):
    return pl.ds(pl.multiple_of(step * width, width), width)


def cuts(total, *shares):
    whole, at, parts = sum(shares), 0, []
    for k in range(len(shares)):
        end = -(-total * sum(shares[: k + 1]) // whole)
        if end > at:
            parts.append((at, end - at))
        at = end
    return parts


def concat(ref, n):
    return jnp.concatenate([ref[j] for j in range(n)], axis=-1)


shape = jax.ShapeDtypeStruct
any_, whole = pl.BlockSpec(memory_space=pl.ANY), pl.BlockSpec(memory_space=pltpu.VMEM)


def two(*dims, dtype=BF16):
    return pltpu.VMEM((PAIR, *dims), dtype)


class Sizes:
    def __init__(self, shares, tokens, d, ff):
        self.tokens, self.d, self.ff, self.half = tokens, d, ff, d // PAIR
        self.tiles, self.rd, self.rf = ff // TILE, d // DEVICES, ff // DEVICES
        self.parts = cuts(self.tiles, *shares)
        self.deep, self.tall, self.wide = (self.tiles, *GRID, self.rd, TILE), (ff, d), (self.tiles, tokens, TILE)
        self.thin, self.turned = (tokens, d), (d, tokens)
        self.blocks = [shape((self.rd, ff), BF16)] * PAIR + [shape((self.rf, d), BF16)]
        slots = Scatter.scratch(1, self.rf, self.half) * PAIR
        for _, size in self.parts:
            slots += Scatter.scratch(size, self.rd, TILE) * PAIR
        self.n_slots = PAIR + PAIR * len(self.parts)
        self.slot_size, self.slots = len(slots) // self.n_slots, slots
        many = PAIR if tokens % (PAIR * LINE * TILE) == 0 else 1
        self.halves = [pl.ds(q * (tokens // many), tokens // many) for q in range(many)]
        self.hidden_bufs = [two(tokens, TILE, dtype=F32)] * PAIR + [two(TILE, d)] + [two(tokens, TILE)] * PAIR
        self.hidden_bufs += [two(*GRID, self.rd, TILE)] * PAIR


def block_rows(plane, z, c, r):
    return pl.ds(pl.multiple_of(((plane * LINE + z) * PAIR + c) * r, 8), r)


def piece(refs, bufs, sems):
    return [(lambda s, ref=ref: ref.at[s], buf, sems.at[k]) for k, (ref, buf) in enumerate(zip(refs, bufs))]


def scatters(place, pump, size, slots, sems, acc, out, down, wide, tempo):
    state = {"free": 0.0}

    def scatter(n, terms, to, slot, share):
        one = Scatter(place, n, terms, to, slots[slot], sems.at[slot], acc)
        matrix, head, tail = tempo
        wire = matrix * share

        def put():
            now = pump.now
            start = max(now + 3, state["free"])
            state["free"] = start + wire
            ahead, end = max(now + 3, start - head), start + tail * wire + 5
            acts = [(now, one.start), (ahead, one.diagonal), (ahead, one.straight), (start + 0.4 * wire, one.joined)]
            acts += [(start + wire + 2, one.along_z), (end, one.last), (end, one.sent)]
            for when, act in acts:
                pump.insert(when, act)

        return put

    def down_job(k):
        part = pl.ds(k * size.half, size.half)
        terms = lambda plane, c: [(down.at[block_rows(plane, z, c, size.rf), part], lambda to, z=z: to.at[0, z]) for z in range(LINE)]
        return scatter(1, terms, lambda i: out[-1].at[:, part], k, 0.5)

    def wide_job(b, k):
        start, n = size.parts[b]
        terms = lambda plane, c: [(wide[k].at[pl.ds(start, n), plane, :, c], lambda to: to)]
        to = lambda i: out[k].at[:, pl.ds((start + i) * TILE, TILE)]
        return scatter(n, terms, to, PAIR + PAIR * b + k, n / size.tiles)

    jobs = [[down_job(k) for k in range(PAIR)]] + [[wide_job(b, k) for k in range(PAIR)] for b in range(len(size.parts))]

    def put_all(puts):
        for put in puts:
            put()

    return [functools.partial(put_all, puts) for puts in jobs]


def hidden(size, pump, by, at, ins, grads, kept, held, puts, cost, before, sems, gbuf, ubuf, wdbuf, dgbuf, dubuf, gout, uout):
    in_sem, out_sem = sems
    gate, up, w_down = ins
    dg, du = held or (dgbuf.at[0], dubuf.at[0])

    def body(step, ins, outs):
        for part in size.halves:
            by_act = nt(by[part, :], ins[2][:]).astype(BF16).astype(F32)
            dg[part, :], du[part, :] = both = silu_back(ins[0][part, :], ins[1][part, :], by_act)
            for out, value in zip(outs[PAIR:], both):
                out[part, :] = value
        for out, grad in zip(outs, (dg, du)):
            out[:] = nn(at[:], grad[:]).astype(BF16).reshape(*GRID, size.rd, TILE)

    outs = piece((*grads, *kept), (gout, uout, dgbuf, dubuf)[: PAIR + len(kept)], out_sem)
    inject = {min(start + n, size.tiles - 1): [put] for (start, n), put in zip(size.parts, puts[:-1])}
    streams = piece((gate, up), (gbuf, ubuf), in_sem)
    streams.append((lambda s: w_down.at[cols(s, TILE), :], wdbuf, in_sem.at[2]))
    stream(size.tiles, streams, outs, body, lambda: pump.plan(size.tiles, cost, inject=inject), before=before)
    puts[-1]()
    run(pump.due())


def first_part(x, dy, weights):
    size = Sizes(SHARES[1], *x.shape, weights[0].shape[-1])
    tokens, d, ff, tiles, rd, rf, half = size.tokens, size.d, size.ff, size.tiles, size.rd, size.rf, size.half
    rows, few = tokens // LINE, tokens // (PAIR * LINE)
    chunks = [cuts(tiles, *shares) for shares in SHARES[0]]
    jobs_of, gates = [], [{}, {}]
    for layer in range(PAIR):
        for start, n in chunks[layer]:
            if layer and start == chunks[1][-1][0]:
                jobs_of.append((1, 2, 0, half))
            jobs_of += [(layer, 0, start, n), (layer, 1, start, n)]
            gates[layer][start] = len(jobs_of) - 1
        jobs_of += [(1, 2, half, half)] if layer else [(0, 2, 0, half), (0, 2, half, half)]
        gates[layer]["down"] = len(jobs_of) - 1
    nj = len(jobs_of)
    held_shapes = [(PAIR, tiles, rd, TILE), (PAIR, tiles, rd, TILE), (PAIR, rf, d)]
    deep, tall, wide, thin, turned = size.deep, size.tall, size.wide, size.thin, size.turned
    hbm = [turned, wide, deep, deep, tall, deep, deep, tall, thin, tall, wide, wide, deep, deep]
    hbm = [shape(thin, BF16), shape(tall, BF16), shape(wide, F32), shape(wide, F32)] + [shape(dims, BF16) for dims in hbm]
    hbm += [shape(wide, F32)] * PAIR
    scratch = [pltpu.VMEM(dims, BF16) for dims in held_shapes + [thin, thin, turned, deep]]

    def kernel(*refs):
        it = iter(refs)
        take = lambda n: [next(it) for _ in range(n)]
        x_hbm, dy_hbm, *w_hbm = take(PAIR + len(weights))
        *out, acc = take(len(weights) + 1)
        dh1, dwd0, gate0, up0, a0t, act0, g0, u0, d0, g1, u1, d1, h1_hbm, dwd1, dg1, du1, dwg1, dwu1, gate1, up1 = take(len(hbm))
        full = [[g0, u0, d0], [g1, u1, d1]]
        *held, a, by, at, wg = take(len(scratch))
        slots = [take(size.slot_size) for _ in range(size.n_slots)]
        load_sem, ag_sems, rs_sems, in_sem, out_sem, one_sem = take(6)
        s_x, s_at, s_w, s_u = (one_sem.at[k] for k in range(4))
        place = Place()

        def load(k, layer):
            ref, sem = w_hbm[k].at[layer], load_sem.at[k, layer]
            if k == PAIR:
                pltpu.make_async_copy(ref, held[k].at[layer], sem).start()
            else:
                for t in range(tiles):
                    pltpu.make_async_copy(ref.at[:, pl.ds(TILE * t, TILE)], held[k].at[layer, t], sem).start()

        x_load = pltpu.make_async_copy(x_hbm, by, s_x)
        greeting = greet(place.sharers)
        for layer in range(PAIR):
            for k in range(len(held)):
                load(k, layer)
                if k == 1 and not layer:
                    x_load.start()
        greeting()
        acc[:] = jnp.zeros_like(acc)
        pump, jobs, loaded = Pump(), [], set()

        def first(j):
            layer, k, _, _ = jobs_of[j]
            if (k, layer) not in loaded:
                await_bytes(held[k].at[layer], load_sem.at[k, layer])
                loaded.add((k, layer))
            jobs[j].z_first()

        clock = begun = 4.0
        for j, (layer, k, start, n) in enumerate(jobs_of):
            part, ref = pl.ds(start, n), full[layer][k]
            if k == PAIR:

                def blocks(plane, zs, c, ref=ref, part=part):
                    zs = [zs.start + i for i in range(zs.size)] if isinstance(zs, pl.Slice) else [zs]
                    return [ref.at[block_rows(plane, z, c, rf), part] for z in zs]

                amount = lambda n, ref=ref, part=part: ref.at[pl.ds(0, n * rf), part]
                mine = held[k].at[layer, :, part]
            else:
                blocks = lambda plane, zs, c, ref=ref, part=part: [ref.at[part, plane, zs, c]]
                amount = lambda n, ref=ref, part=part: ref.at[part, pl.ds(0, max(1, n // LINE)), pl.ds(0, min(n, LINE)), 0]
                mine = held[k].at[layer, part]
            job = Gather(place, mine, blocks, amount, ag_sems.at[j], j < PAIR)
            jobs.append(job)
            took = TOOK * n / (d if k == PAIR else tiles)
            unit = took / 6
            lead = min(max(0.33 * clock - 5, 3), LEAD)
            zero = begun - 4
            pump.insert(zero, functools.partial(first, j))
            if not job.direct:
                pump.insert(zero + unit + 2.5, job.z_second)
                pump.insert(zero + 3 * unit + 5, job.z_third)
            ready = max(zero + 5 * unit + (5 if job.direct else 7.5), clock - lead)
            clock = max(clock, ready)
            pump.insert(ready, job.plane)
            pump.insert(clock + 0.4 * took, job.across)
            pump.insert(clock + 0.75 * took, job.to_core)
            behind = PAIR if j >= nj - 3 else lead
            pump.insert(clock + took + behind + 1, job.last_to_core)
            pump.insert(clock + took + behind + 2, job.done, j)
            clock += took
            begun += (PACE if j > 1 else DIRECT) * took
        pump.now = 3.0
        run(pump.due())
        x_load.wait()
        a0_out = pltpu.make_async_copy(at, a0t, s_at)
        dy_load = pltpu.make_async_copy(dy_hbm, by, s_x)

        step = min(TILE, tokens)

        def norm(i, _):
            part = cols(i, step)
            normed = norm_rows(by[part, :])
            a[part, :] = normed
            at[:, part] = normed.T
            return 0

        lax.fori_loop(0, tokens // step, norm, 0)
        a0_out.start()
        pump.now = 8.0

        def gate_up(layer, gate, up, before, wgate, wup, gbuf, ubuf, actbuf, dwbuf):
            def body(step, ins, outs):
                g = nn(a[:], ins[0][:].reshape(d, TILE))
                u = nn(a[:], ins[1][:].reshape(d, TILE))
                outs[0][:] = g
                outs[1][:] = u
                product = (g * jax.nn.sigmoid(g) * u).astype(BF16)
                if layer:
                    actbuf[0] = product
                    outs[2][:] = tn(actbuf[0], by[:]).astype(BF16)
                else:
                    outs[2][:] = product

            run(pump.through(gates[layer][0]))
            later = {s: j for s, j in gates[layer].items() if s in range(1, tiles)}
            outs = piece((gate, up, act0), (gbuf, ubuf, actbuf), out_sem)
            if layer:
                outs[-1] = (lambda s: dwd1.at[cols(s, TILE), :], dwbuf, out_sem.at[2])
            stream(
                tiles,
                piece(full[layer][:PAIR], (wgate, wup), in_sem),
                outs,
                body,
                lambda: pump.plan(tiles, 3.7 if layer else 2.5, later),
                late=[s - 1 for s in later],
                before=before,
            )

        def down(wd, tall, hbuf):
            run(pump.through(gates[0]["down"]))
            wd_load = pltpu.make_async_copy(d0, wd, s_w)
            wd_load.start()

            def ready():
                a0_out.wait()
                wd_load.wait()

            def body(step, ins, outs):
                part = cols(step, rows)
                h = by[part, :] + nn(concat(ins[0], tiles), wd[:]).astype(BF16)
                outs[0][:] = h
                normed = norm_rows(h)
                a[part, :] = normed
                at[:, part] = normed.T

            stream(
                tokens // rows,
                [(lambda s: act0.at[:, cols(s, rows), :], tall, in_sem.at[0])],
                [(lambda s: h1_hbm.at[cols(s, rows), :], hbuf, out_sem.at[0])],
                body,
                lambda: pump.plan(tokens // rows, 3.8),
                before=ready,
            )
            dy_load.start()

        tile_bufs = [two(*GRID, rd, TILE)] * PAIR + [two(tokens, TILE, dtype=F32)] * PAIR + [two(tokens, TILE), two(TILE, d)]
        pl.run_scoped(functools.partial(gate_up, 0, gate0, up0, None), *tile_bufs)
        pl.run_scoped(down, pltpu.VMEM(d0.shape, BF16), two(tiles, rows, TILE), two(rows, d))
        pl.run_scoped(functools.partial(gate_up, 1, gate1, up1, dy_load.wait), *tile_bufs)
        run(pump.through(nj - 1))
        assert not pump.items
        put_down, *put_wide = scatters(place, pump, size, slots, rs_sems, acc, out, dwd1, (dwg1, dwu1), TEMPOS[0])
        put_down()
        run(pump.due())
        wg_load = pltpu.make_async_copy(g1, wg, s_w)
        wg_load.start()
        ins, grads = (gate1, up1, d1), (dwg1, dwu1)
        room = [a.at[:, pl.ds(k * TILE, TILE)] for k in range(PAIR)]
        pl.run_scoped(
            functools.partial(hidden, size, pump, by, at, ins, grads, (dg1, du1), room, put_wide, HID1, None, (in_sem, out_sem)), *size.hidden_bufs
        )

        def states(wu, dgbuf, dubuf, hbuf):
            wu_load = pltpu.make_async_copy(u1, wu, s_u)
            wu_load.start()

            def ready():
                wg_load.wait()
                wu_load.wait()

            def body(step, ins, outs):
                part = cols(step, few)
                dg, du, h = (ref for ref in ins)
                da = nt(concat(dg, tiles), concat(wg, tiles).reshape(d, ff)) + nt(concat(du, tiles), concat(wu, tiles).reshape(d, ff))
                by[part, :] = by[part, :] + norm_back(da.astype(BF16), h[:])

            ins = [(lambda s, ref=ref: ref.at[:, cols(s, few), :], buf, in_sem.at[k]) for k, (ref, buf) in enumerate(((dg1, dgbuf), (du1, dubuf)))]
            ins.append((lambda s: h1_hbm.at[cols(s, few), :], hbuf, in_sem.at[2]))
            stream(tokens // few, ins, [], body, lambda: pump.plan(tokens // few, STATES), before=ready)

        pl.run_scoped(states, pltpu.VMEM(wg.shape, BF16), two(tiles, few, TILE), two(tiles, few, TILE), two(few, d))
        by_out = pltpu.make_async_copy(by, dh1, s_x)
        by_out.start()

        def down_gradient(abuf, wbuf):
            def body(step, ins, outs):
                outs[0][:] = tn(ins[0][:], by[:]).astype(BF16)

            outs = [(lambda s: dwd0.at[cols(s, TILE), :], wbuf, out_sem.at[0])]
            stream(tiles, piece((act0,), (abuf,), in_sem), outs, body, lambda: pump.plan(tiles, 1.4))

        pl.run_scoped(down_gradient, two(tokens, TILE), two(TILE, d))
        pump.now = 1e9
        run(pump.due())
        for job in jobs:
            job.sent()
        by_out.wait()

    DMA = pltpu.SemaphoreType.DMA
    outs = pl.pallas_call(
        kernel,
        name="first_part",
        in_specs=[any_] * (PAIR + len(weights)),
        out_specs=[whole] * (len(weights) + 1) + [any_] * len(hbm),
        out_shape=size.blocks + [shape((8, LANES), F32)] + hbm,
        scratch_shapes=scratch
        + size.slots
        + [DMA((3, PAIR)), DMA((nj, len(Gather.SLOTS))), DMA((size.n_slots, len(Scatter.SLOTS)))]
        + [DMA((4, PAIR)), DMA((4, PAIR)), DMA((4,))],
        compiler_params=pltpu.CompilerParams(collective_id=0, has_side_effects=True, vmem_limit_bytes=66_500_000),
    )(x, dy, *weights)
    *sums, acc = outs[: len(weights) + 1]
    dh1, dwd0, gate0, up0, a0t, _, _, _, d0 = outs[len(weights) + 1 :][:9]
    return sums, acc, (dh1, dwd0, gate0, up0, a0t, d0)


def second_part(last_acc, dh1, dwd0, gate0, up0, a0t, d0):
    size = Sizes(SHARES[2], *dh1.shape, d0.shape[0])
    deep = shape(size.deep, BF16)
    n = len(size.blocks)

    def kernel(*refs):
        it = iter(refs)
        take = lambda n: [next(it) for _ in range(n)]
        acc_in, dh1_hbm, dwd0, gate0, up0, a0t, d0 = take(7)
        *out, squares = take(n + 1)
        dwg0, dwu0 = take(PAIR)
        by, at = take(PAIR)
        slots = [take(size.slot_size) for _ in range(size.n_slots)]
        acc, sums, gone, rs_sems, in_sem, out_sem, sums_sem, one_sem = take(8)
        place, pump = Place(), Pump()
        by_load, at_load = pltpu.make_async_copy(dh1_hbm, by, one_sem.at[0]), pltpu.make_async_copy(a0t, at, one_sem.at[1])
        by_load.start()
        at_load.start()
        greeting = greet(place.sharers + [place.to_diag])

        def ready():
            greeting()
            put_down()
            run(pump.due())
            acc[:] = acc_in[:]
            by_load.wait()
            at_load.wait()

        put_down, *put_wide = scatters(place, pump, size, slots, rs_sems, acc, out, dwd0, (dwg0, dwu0), TEMPOS[1])
        ins, grads = (gate0, up0, d0), (dwg0, dwu0)
        pl.run_scoped(
            functools.partial(hidden, size, pump, by, at, ins, grads, (), None, put_wide, HID0, ready, (in_sem, out_sem)), *size.hidden_bufs
        )
        pump.now = 1e9
        run(pump.due())
        sums[0] = jnp.full(acc.shape, jnp.sum(acc[:]), F32)
        hops = [[place.to_c], [place.to_x, place.to_y, place.to_diag], place.to_z]
        at_gone = 0
        for k, devices in enumerate(hops):
            for i, device in enumerate(devices):
                send(sums.at[k], gone.at[at_gone + i], sums_sem.at[len(hops)], sums_sem.at[k], device)
            await_bytes(gone.at[pl.ds(at_gone, len(devices))], sums_sem.at[k])
            total = sums[k]
            for i in range(len(devices)):
                total += gone[at_gone + i]
            at_gone += len(devices)
            if k < len(hops) - 1:
                sums[k + 1] = total
            else:
                squares[:] = total
        await_bytes(gone, sums_sem.at[len(hops)])

    DMA = pltpu.SemaphoreType.DMA
    tile = (8, LANES)
    *sums, squares = pl.pallas_call(
        kernel,
        name="second_part",
        in_specs=[whole] + [any_] * 6,
        out_specs=[whole] * (n + 1) + [any_] * PAIR,
        out_shape=size.blocks + [shape(tile, F32)] + [deep, deep],
        scratch_shapes=[pltpu.VMEM(size.thin, BF16), pltpu.VMEM(size.turned, BF16)]
        + size.slots
        + [pltpu.VMEM(tile, F32), pltpu.VMEM((3, *tile), F32), pltpu.VMEM((7, *tile), F32)]
        + [DMA((size.n_slots, len(Scatter.SLOTS))), DMA((4, PAIR)), DMA((4, PAIR)), DMA((4,)), DMA((PAIR,))],
        compiler_params=pltpu.CompilerParams(collective_id=1, has_side_effects=True, vmem_limit_bytes=66_500_000),
    )(last_acc, dh1, dwd0, gate0, up0, a0t, d0)[: n + 1]
    return sums, squares


def adamw(weights, m, v, sums, squares):
    n = len(weights)
    count = DEVICES * sum(w.size for w in weights)

    def kernel(squares_ref, *refs):
        factor = jnp.minimum(1.0, 0.5 * lax.rsqrt(squares_ref[:1, :1] / count + 1e-30))
        for k in range(n):
            w, m, v, g, last_g, new_w, new_m, new_v = refs[k::n]
            grad = jnp.where(pl.program_id(0) == 0, g[:].astype(F32), last_g[:].astype(F32)) * factor
            m_next = 0.9 * m[0] + 0.1 * grad
            v_next = 0.95 * v[0] + 0.05 * grad * grad
            wide = w[0].astype(F32)
            new_w[0] = (wide - 0.02 * (m_next * lax.rsqrt(v_next + 1e-8) + 0.1 * wide)).astype(BF16)
            new_m[0] = m_next
            new_v[0] = v_next

    blocks = [pl.BlockSpec((1, *w.shape[1:]), lambda layer: (layer, 0, 0)) for w in weights]
    once = [pl.BlockSpec(s.shape, lambda layer: (0, 0)) for s in (squares, *sums)]
    return pl.pallas_call(
        kernel,
        name="adamw",
        grid=(PAIR,),
        in_specs=once[:1] + blocks * 3 + once[1:],
        out_specs=blocks * 3,
        out_shape=[shape(w.shape, BF16) for w in weights] + [shape(w.shape, F32) for w in weights] * PAIR,
    )(squares, *weights, *m, *v, *sums)


def solution(mesh):
    def step(x, dy, *arrays):
        weights, m, v = (arrays[3 * i : 3 * i + 3] for i in range(3))
        last, acc, kept = first_part(x[0], dy[0], weights)
        sums, squares = second_part(acc, *kept)
        return tuple(adamw(weights, m, v, [*sums, *last], squares))

    states, cut = P(("rep", "dp"), None, None), P(None, "dp", None)
    return jax.shard_map(
        step,
        mesh=mesh,
        in_specs=(states, states) + (cut,) * 9,
        out_specs=(P("rep", "dp", None),) * 9,
        check_vma=False,
    )
```

```python
import functools

import jax
import jax.numpy as jnp
from jax import lax
from jax.experimental import pallas as pl
from jax.experimental.pallas import tpu as pltpu
from jax.sharding import PartitionSpec as P

F32, BF16 = jnp.float32, jnp.bfloat16
MESH = pl.DeviceIdType.MESH
DEVICES, PLANE, LINE, TILE, LANES = 32, 4, 4, 256, 128
PAIR = 2
LO, HI, ALL = pl.ds(0, PAIR), pl.ds(PAIR, PAIR), pl.ds(0, LINE)
GRID = (PLANE, LINE, PAIR)
LEAD, TOOK = 14, 24.0
TEMPOS = (25.0, 4, 1.6), (25.0, 6, 1.6)
STATES, HID1, HID0 = 3.6, 4.4, 3.9
DIRECT, PACE = 0.5, 0.5
SHARES = ((3, 4, 4), (3, 3, 3, 2)), (3, 3, 3, 2), (2, 3, 3, 3)


def nn(a, b):
    return jnp.dot(a, b, preferred_element_type=F32)


def tn(a, b):
    return lax.dot_general(a, b, (((0,), (0,)), ((), ())), preferred_element_type=F32)


def nt(a, b):
    return lax.dot_general(a, b, (((1,), (1,)), ((), ())), preferred_element_type=F32)


def norm_scale(wide):
    return lax.rsqrt(jnp.mean(wide * wide, -1, keepdims=True) + 1e-6)


def norm_rows(h):
    wide = h.astype(F32)
    return (wide * norm_scale(wide)).astype(BF16)


def norm_back(da, h):
    wide, da = h.astype(F32), da.astype(F32)
    scale = norm_scale(wide)
    return (da * scale - wide * (scale * scale * scale * jnp.mean(da * wide, -1, keepdims=True))).astype(BF16)


def silu_back(gate, up, by_act):
    s = jax.nn.sigmoid(gate)
    return (by_act * up * s * (1 + gate * (1 - s))).astype(BF16), (by_act * gate * s).astype(BF16)


class Place:
    def __init__(self):
        d = lax.axis_index("dp")
        self.c, chip = d % PAIR, d // PAIR
        self.z, self.own = chip % LINE, chip // LINE
        x, y = self.own // PAIR, self.own % PAIR
        self.xs, self.ys, self.diag = (1 - x) * PAIR + y, x * PAIR + 1 - y, (1 - x) * PAIR + 1 - y
        self.near, self.far = pl.ds(self.z // PAIR * PAIR, PAIR), pl.ds(PAIR - self.z // PAIR * PAIR, PAIR)
        self.inner = jnp.logical_or(self.z == 1, self.z == 2)
        self.outer = jnp.logical_not(self.inner)
        at = lambda plane, z, c: {"dp": (plane * LINE + z) * PAIR + c}
        self.to_x, self.to_y, self.to_diag = (at(plane, self.z, self.c) for plane in (self.xs, self.ys, self.diag))
        self.to_c = at(self.own, self.z, 1 - self.c)
        self.to_z = [at(self.own, (self.z + k) % LINE, self.c) for k in range(1, LINE)]
        self.next_z = at(self.own, self.z + 1 - PAIR * (self.z % PAIR), self.c)
        self.across_z = at(self.own, LINE - 1 - self.z, self.c)
        self.sharers = [self.to_x, self.to_y, self.to_c, *self.to_z]


def signal_all(sem, devices):
    for device in devices:
        pl.semaphore_signal(sem, inc=1, device_id=device, device_id_type=MESH)


def greet(devices):
    barrier = pltpu.get_barrier_semaphore()
    signal_all(barrier, devices)
    return lambda: pl.semaphore_wait(barrier, len(devices))


def send(src, dst, send_sem, recv_sem, device):
    pltpu.make_async_remote_copy(src, dst, send_sem, recv_sem, device_id=device, device_id_type=MESH).start()


def await_bytes(ref, sem):
    pltpu.make_async_copy(ref, ref, sem).wait()


class Gather:
    Z, Z2, Z3, XA, XB, YA, YB, DX, DY, C, OWN, SENT = SLOTS = range(12)

    def __init__(self, place, mine, blocks, amount, sems, direct):
        self.p, self.mine, self.blocks, self.amount, self.sems, self.direct = place, mine, blocks, amount, sems, direct

    def z_first(self):
        p = self.p
        (here,) = self.blocks(p.own, p.z, p.c)
        pltpu.make_async_copy(self.mine, here, self.sems.at[self.OWN]).start()
        for device in p.to_z if self.direct else [p.next_z]:
            send(self.mine, here, self.sems.at[self.SENT], self.sems.at[self.Z], device)

    def _move(self, plane, zs, slot, device):
        for ref in self.blocks(plane, zs, self.p.c):
            send(ref, ref, self.sems.at[self.SENT], self.sems.at[slot], device)

    def _wait(self, slot, blocks=PAIR):
        await_bytes(self.amount(blocks), self.sems.at[slot])

    def z_second(self):
        @pl.when(self.p.inner)
        def _():
            self._wait(self.Z, 1)
            self._wait(self.OWN, 1)
            self._move(self.p.own, self.p.near, self.Z2, self.p.across_z)

    def z_third(self):
        @pl.when(self.p.inner)
        def _():
            self._wait(self.Z2)
            self._move(self.p.own, self.p.far, self.Z3, self.p.next_z)

    def plane(self):
        p = self.p
        if self.direct:
            self._wait(self.Z, LINE - 1)
            self._wait(self.OWN, 1)
        else:

            @pl.when(p.outer)
            def _():
                self._wait(self.Z, 1)
                self._wait(self.OWN, 1)
                self._wait(self.Z3)

        self._move(p.own, LO, self.XA, p.to_x)
        self._move(p.own, HI, self.YB, p.to_y)
        self._move(p.own, HI, self.XB, p.to_x)
        self._move(p.own, LO, self.YA, p.to_y)
        self._move(p.own, ALL, self.C, p.to_c)

    def across(self):
        p = self.p
        self._wait(self.XA)
        self._move(p.xs, LO, self.DY, p.to_y)
        self._wait(self.YB)
        self._move(p.ys, HI, self.DX, p.to_x)

    def to_core(self):
        p = self.p
        self._wait(self.XB)
        self._move(p.xs, ALL, self.C, p.to_c)
        self._wait(self.YA)
        self._move(p.ys, ALL, self.C, p.to_c)

    def last_to_core(self):
        self._wait(self.DY)
        self._wait(self.DX)
        self._move(self.p.diag, ALL, self.C, self.p.to_c)

    def done(self):
        self._wait(self.C, PLANE * LINE)

    def sent(self):
        for _ in range(LINE - 1 if self.direct else 1):
            await_bytes(self.mine, self.sems.at[self.SENT])
        if not self.direct:
            pl.when(self.p.inner)(functools.partial(self._wait, self.SENT, LINE))
        for blocks in (PLANE, PLANE - 1):
            self._wait(self.SENT, blocks * LINE)


def add_into(dst, *srcs):
    def one(i, _):
        for z in range(dst.shape[1]):
            total = srcs[0][i, z].astype(F32)
            for s in srcs[1:]:
                total += s[i, z].astype(F32)
            dst[i, z] = total.astype(dst.dtype)
        return 0

    if dst.shape[0] == 1:
        one(0, 0)
    else:
        lax.fori_loop(0, dst.shape[0], one, 0)


class Scatter:
    P1X, P1Y, XA, XB, YA, YB, Z, SENT, *C, L0, L1, L2, L3 = SLOTS = range(16)
    L = (L0, L1, L2, L3)

    @staticmethod
    def scratch(n, r, w):
        return [pltpu.VMEM(s + (r, w), BF16) for s in ((PLANE, n, LINE), (PLANE, n, LINE), (n, 3 * LINE), (LINE - 1, n))]

    def __init__(self, place, n, terms, out, slot, sems, acc):
        self.p, self.n, self.terms, self.out, self.sems, self.acc = place, n, terms, out, sems, acc
        mine, other, arrived, rz = slot
        some = pl.ds(0, n)
        self.mine, self.other = (lambda g, zs=ALL: mine.at[g, some, zs]), (lambda g, zs=ALL: other.at[g, some, zs])
        self.p1x, self.p1y = arrived.at[some, LO], arrived.at[some, HI]
        self.rx, self.ry = (lambda lo: arrived.at[some, pl.ds(LINE + lo, PAIR)]), (lambda lo: arrived.at[some, pl.ds(PAIR * LINE + lo, PAIR)])
        self.rz, self.kept = rz.at[:, some], mine

    def start(self):
        p = self.p
        for g, plane in enumerate((p.diag, p.xs, p.ys, p.own)):
            for ref, part in self.terms(plane, 1 - p.c):
                send(ref, part(self.other(g)), self.sems.at[self.SENT], self.sems.at[self.C[g]], p.to_c)
            for ref, part in self.terms(plane, p.c):
                pltpu.make_async_copy(ref, part(self.mine(g)), self.sems.at[self.L[g]]).start()

    def _both(self, g):
        await_bytes(self.other(g), self.sems.at[self.C[g]])
        await_bytes(self.mine(g), self.sems.at[self.L[g]])

    def _send(self, src, dst, slot, device):
        send(src, dst, self.sems.at[self.SENT], self.sems.at[slot], device)

    def diagonal(self):
        p = self.p
        self._both(0)
        add_into(self.mine(0), self.mine(0), self.other(0))
        self._send(self.mine(0, LO), self.p1x, self.P1X, p.to_x)
        self._send(self.mine(0, HI), self.p1y, self.P1Y, p.to_y)

    def straight(self):
        p = self.p
        self._both(1)
        add_into(self.mine(1, LO), self.mine(1, LO), self.other(1, LO))
        self._send(self.mine(1, LO), self.rx(0), self.XA, p.to_x)
        self._both(2)
        add_into(self.mine(2, HI), self.mine(2, HI), self.other(2, HI))
        self._send(self.mine(2, HI), self.ry(PAIR), self.YB, p.to_y)

    def joined(self):
        p = self.p
        await_bytes(self.p1y, self.sems.at[self.P1Y])
        add_into(self.mine(1, HI), self.mine(1, HI), self.other(1, HI), self.p1y)
        self._send(self.mine(1, HI), self.rx(PAIR), self.XB, p.to_x)
        await_bytes(self.p1x, self.sems.at[self.P1X])
        add_into(self.mine(2, LO), self.mine(2, LO), self.other(2, LO), self.p1x)
        self._send(self.mine(2, LO), self.ry(0), self.YA, p.to_y)

    def along_z(self):
        p = self.p
        self._both(3)
        for part, lo, xs, ys in ((LO, 0, self.XA, self.YA), (HI, PAIR, self.XB, self.YB)):
            await_bytes(self.rx(lo), self.sems.at[xs])
            await_bytes(self.ry(lo), self.sems.at[ys])
            add_into(self.mine(3, part), self.mine(3, part), self.other(3, part), self.rx(lo), self.ry(lo))
        for k, device in enumerate(p.to_z):
            self._send(self.mine(3, (p.z + 1 + k) % LINE), self.rz.at[k], self.Z, device)

    def last(self):
        await_bytes(self.rz, self.sems.at[self.Z])
        for i in range(self.n):
            total = self.kept[3, i, self.p.z].astype(F32)
            for k in range(LINE - 1):
                total += self.rz[k, i].astype(F32)
            g = total.astype(BF16)
            self.out(i)[:] = g
            g = g.astype(F32)
            g = g * g
            r, w = g.shape
            lanes = g[:, :LANES]
            for k in range(1, w // LANES):
                lanes += g[:, LANES * k : LANES * (k + 1)]
            self.acc[:] += jnp.sum(lanes.reshape(-1, *self.acc.shape), 0)

    def sent(self):
        for _ in range(7):
            await_bytes(self.other(0), self.sems.at[self.SENT])
        await_bytes(self.rz, self.sems.at[self.SENT])


class Pump:
    def __init__(self):
        self.items, self.now = [], 0.0

    def insert(self, when, act, tag=None):
        at = len(self.items)
        while at and self.items[at - 1][0] > when:
            at -= 1
        self.items.insert(at, (when, act, tag))

    def due(self):
        acts = []
        while self.items and self.items[0][0] <= self.now:
            acts.append(self.items.pop(0)[1])
        return acts

    def through(self, tag):
        acts = []
        while any(t == tag for _, _, t in self.items):
            when, act, _ = self.items.pop(0)
            self.now = max(self.now, when)
            acts.append(act)
        return acts

    def plan(self, steps, cost, gates=None, inject=None):
        ticks = {}
        for s in range(steps):
            self.now += cost
            if inject and s in inject:
                for put in inject[s]:
                    put()
            acts = self.due()
            if gates and s + 1 in gates:
                acts += self.through(gates[s + 1])
            if acts:
                ticks[s] = acts
        return ticks


def run(acts):
    for act in acts:
        act()


def stream(steps, ins, outs, body, ticks, late=(), before=None):
    def fetch(step):
        for where, buf, sem in ins:
            pltpu.make_async_copy(where(step), buf.at[step % PAIR], sem.at[step % PAIR]).start()

    def one(step, _):
        slot = step % PAIR
        early = step + 1 < steps
        for t in late:
            early = jnp.logical_and(early, step != t)
        pl.when(early)(lambda: fetch(step + 1))
        for _, buf, sem in ins:
            await_bytes(buf.at[slot], sem.at[slot])
        body(step, [buf.at[slot] for _, buf, _ in ins], [buf.at[slot] for _, buf, _ in outs])

        @pl.when(step >= 1)
        def _():
            for _, buf, sem in outs:
                await_bytes(buf.at[1 - slot], sem.at[1 - slot])

        for where, buf, sem in outs:
            pltpu.make_async_copy(buf.at[slot], where(step), sem.at[slot]).start()
        for t, acts in plan.items():
            pl.when(step == t)(functools.partial(run, acts))
        for t in late:
            pl.when(step == t)(lambda t=t: fetch(t + 1))
        return 0

    fetch(0)
    if before is not None:
        before()
    plan = ticks()
    lax.fori_loop(0, steps, one, 0)
    for _, buf, sem in outs:
        await_bytes(buf.at[(steps - 1) % PAIR], sem.at[(steps - 1) % PAIR])


def cols(step, width):
    return pl.ds(pl.multiple_of(step * width, width), width)


def cuts(total, *shares):
    whole, at, parts = sum(shares), 0, []
    for k in range(len(shares)):
        end = -(-total * sum(shares[: k + 1]) // whole)
        if end > at:
            parts.append((at, end - at))
        at = end
    return parts


def concat(ref, n):
    return jnp.concatenate([ref[j] for j in range(n)], axis=-1)


shape = jax.ShapeDtypeStruct
any_, whole = pl.BlockSpec(memory_space=pl.ANY), pl.BlockSpec(memory_space=pltpu.VMEM)


def two(*dims, dtype=BF16):
    return pltpu.VMEM((PAIR, *dims), dtype)


class Sizes:
    def __init__(self, shares, tokens, d, ff):
        self.tokens, self.d, self.ff, self.half = tokens, d, ff, d // PAIR
        self.tiles, self.rd, self.rf = ff // TILE, d // DEVICES, ff // DEVICES
        self.parts = cuts(self.tiles, *shares)
        self.deep, self.tall, self.wide = (self.tiles, *GRID, self.rd, TILE), (ff, d), (self.tiles, tokens, TILE)
        self.thin, self.turned = (tokens, d), (d, tokens)
        self.blocks = [shape((self.rd, ff), BF16)] * PAIR + [shape((self.rf, d), BF16)]
        slots = Scatter.scratch(1, self.rf, self.half) * PAIR
        for _, size in self.parts:
            slots += Scatter.scratch(size, self.rd, TILE) * PAIR
        self.n_slots = PAIR + PAIR * len(self.parts)
        self.slot_size, self.slots = len(slots) // self.n_slots, slots
        many = PAIR if tokens % (PAIR * LINE * TILE) == 0 else 1
        self.halves = [pl.ds(q * (tokens // many), tokens // many) for q in range(many)]
        self.hidden_bufs = [two(tokens, TILE, dtype=F32)] * PAIR + [two(TILE, d)] + [two(tokens, TILE)] * PAIR
        self.hidden_bufs += [two(*GRID, self.rd, TILE)] * PAIR + [pltpu.VMEM((tokens, TILE), BF16)]


def block_rows(plane, z, c, r):
    return pl.ds(pl.multiple_of(((plane * LINE + z) * PAIR + c) * r, 8), r)


def piece(refs, bufs, sems):
    return [(lambda s, ref=ref: ref.at[s], buf, sems.at[k]) for k, (ref, buf) in enumerate(zip(refs, bufs))]


def scatters(place, pump, size, slots, sems, acc, out, down, wide, tempo):
    state = {"free": 0.0}

    def scatter(n, terms, to, slot, share):
        one = Scatter(place, n, terms, to, slots[slot], sems.at[slot], acc)
        matrix, head, tail = tempo
        wire = matrix * share

        def put():
            now = pump.now
            start = max(now + 3, state["free"])
            state["free"] = start + wire
            ahead, end = max(now + 3, start - head), start + tail * wire + 5
            acts = [(now, one.start), (ahead, one.diagonal), (ahead, one.straight), (start + 0.4 * wire, one.joined)]
            acts += [(start + wire + 2, one.along_z), (end, one.last), (end, one.sent)]
            for when, act in acts:
                pump.insert(when, act)

        return put

    def down_job(k):
        part = pl.ds(k * size.half, size.half)
        terms = lambda plane, c: [(down.at[block_rows(plane, z, c, size.rf), part], lambda to, z=z: to.at[0, z]) for z in range(LINE)]
        return scatter(1, terms, lambda i: out[-1].at[:, part], k, 0.5)

    def wide_job(b, k):
        start, n = size.parts[b]
        terms = lambda plane, c: [(wide[k].at[pl.ds(start, n), plane, :, c], lambda to: to)]
        to = lambda i: out[k].at[:, pl.ds((start + i) * TILE, TILE)]
        return scatter(n, terms, to, PAIR + PAIR * b + k, n / size.tiles)

    jobs = [[down_job(k) for k in range(PAIR)]] + [[wide_job(b, k) for k in range(PAIR)] for b in range(len(size.parts))]

    def put_all(puts):
        for put in puts:
            put()

    return [functools.partial(put_all, puts) for puts in jobs]


def hidden(size, pump, by, at, ins, grads, kept, held, puts, cost, before, sems, gbuf, ubuf, wdbuf, dgbuf, dubuf, gout, uout, own):
    in_sem, out_sem = sems
    gate, up, w_down = ins
    dg, du = (own, *held) if held else (dgbuf.at[0], dubuf.at[0])

    def body(step, ins, outs):
        for part in size.halves:
            by_act = nt(by[part, :], ins[2][:]).astype(BF16).astype(F32)
            dg[part, :], du[part, :] = both = silu_back(ins[0][part, :], ins[1][part, :], by_act)
            for out, value in zip(outs[PAIR:], both):
                out[part, :] = value
        for out, grad in zip(outs, (dg, du)):
            out[:] = nn(at[:], grad[:]).astype(BF16).reshape(*GRID, size.rd, TILE)

    outs = piece((*grads, *kept), (gout, uout, dgbuf, dubuf)[: PAIR + len(kept)], out_sem)
    inject = {min(start + n, size.tiles - 1): [put] for (start, n), put in zip(size.parts, puts[:-1])}
    streams = piece((gate, up), (gbuf, ubuf), in_sem)
    streams.append((lambda s: w_down.at[cols(s, TILE), :], wdbuf, in_sem.at[2]))
    stream(size.tiles, streams, outs, body, lambda: pump.plan(size.tiles, cost, inject=inject), before=before)
    puts[-1]()
    run(pump.due())


def first_part(x, dy, weights):
    size = Sizes(SHARES[1], *x.shape, weights[0].shape[-1])
    tokens, d, ff, tiles, rd, rf, half = size.tokens, size.d, size.ff, size.tiles, size.rd, size.rf, size.half
    rows, few = tokens // LINE, tokens // (PAIR * LINE)
    chunks = [cuts(tiles, *shares) for shares in SHARES[0]]
    jobs_of, gates = [], [{}, {}]
    for layer in range(PAIR):
        for start, n in chunks[layer]:
            if layer and start == chunks[1][-1][0]:
                jobs_of.append((1, 2, 0, half))
            jobs_of += [(layer, 0, start, n), (layer, 1, start, n)]
            gates[layer][start] = len(jobs_of) - 1
        jobs_of += [(1, 2, half, half)] if layer else [(0, 2, 0, half), (0, 2, half, half)]
        gates[layer]["down"] = len(jobs_of) - 1
    nj = len(jobs_of)
    held_shapes = [(PAIR, tiles, rd, TILE), (PAIR, tiles, rd, TILE), (PAIR, rf, d)]
    deep, tall, wide, thin, turned = size.deep, size.tall, size.wide, size.thin, size.turned
    hbm = [turned, wide, deep, deep, tall, deep, deep, tall, thin, tall, wide, wide, deep, deep]
    hbm = [shape(thin, BF16), shape(tall, BF16), shape(wide, F32), shape(wide, F32)] + [shape(dims, BF16) for dims in hbm]
    hbm += [shape(wide, F32)] * PAIR
    scratch = [pltpu.VMEM(dims, BF16) for dims in held_shapes + [thin, thin, turned, deep]]

    def kernel(*refs):
        it = iter(refs)
        take = lambda n: [next(it) for _ in range(n)]
        x_hbm, dy_hbm, *w_hbm = take(PAIR + len(weights))
        *out, acc = take(len(weights) + 1)
        dh1, dwd0, gate0, up0, a0t, act0, g0, u0, d0, g1, u1, d1, h1_hbm, dwd1, dg1, du1, dwg1, dwu1, gate1, up1 = take(len(hbm))
        full = [[g0, u0, d0], [g1, u1, d1]]
        *held, a, by, at, wg = take(len(scratch))
        slots = [take(size.slot_size) for _ in range(size.n_slots)]
        load_sem, ag_sems, rs_sems, in_sem, out_sem, one_sem = take(6)
        s_x, s_at, s_w, s_u = (one_sem.at[k] for k in range(4))
        place = Place()

        def load(k, layer):
            ref, sem = w_hbm[k].at[layer], load_sem.at[k, layer]
            if k == PAIR:
                pltpu.make_async_copy(ref, held[k].at[layer], sem).start()
            else:
                for t in range(tiles):
                    pltpu.make_async_copy(ref.at[:, pl.ds(TILE * t, TILE)], held[k].at[layer, t], sem).start()

        x_load = pltpu.make_async_copy(x_hbm, by, s_x)
        greeting = greet(place.sharers)
        for layer in range(PAIR):
            for k in range(len(held)):
                load(k, layer)
                if k == 1 and not layer:
                    x_load.start()
        greeting()
        acc[:] = jnp.zeros_like(acc)
        pump, jobs, loaded = Pump(), [], set()

        def first(j):
            layer, k, _, _ = jobs_of[j]
            if (k, layer) not in loaded:
                await_bytes(held[k].at[layer], load_sem.at[k, layer])
                loaded.add((k, layer))
            jobs[j].z_first()

        clock = begun = 4.0
        for j, (layer, k, start, n) in enumerate(jobs_of):
            part, ref = pl.ds(start, n), full[layer][k]
            if k == PAIR:

                def blocks(plane, zs, c, ref=ref, part=part):
                    zs = [zs.start + i for i in range(zs.size)] if isinstance(zs, pl.Slice) else [zs]
                    return [ref.at[block_rows(plane, z, c, rf), part] for z in zs]

                amount = lambda n, ref=ref, part=part: ref.at[pl.ds(0, n * rf), part]
                mine = held[k].at[layer, :, part]
            else:
                blocks = lambda plane, zs, c, ref=ref, part=part: [ref.at[part, plane, zs, c]]
                amount = lambda n, ref=ref, part=part: ref.at[part, pl.ds(0, max(1, n // LINE)), pl.ds(0, min(n, LINE)), 0]
                mine = held[k].at[layer, part]
            job = Gather(place, mine, blocks, amount, ag_sems.at[j], j < PAIR)
            jobs.append(job)
            took = TOOK * n / (d if k == PAIR else tiles)
            unit = took / 6
            lead = min(max(0.33 * clock - 5, 3), LEAD)
            zero = begun - 4
            pump.insert(zero, functools.partial(first, j))
            if not job.direct:
                pump.insert(zero + unit + 2.5, job.z_second)
                pump.insert(zero + 3 * unit + 5, job.z_third)
            ready = max(zero + 5 * unit + (5 if job.direct else 7.5), clock - lead)
            clock = max(clock, ready)
            pump.insert(ready, job.plane)
            pump.insert(clock + 0.4 * took, job.across)
            pump.insert(clock + 0.75 * took, job.to_core)
            behind = PAIR if j >= nj - 3 else lead
            pump.insert(clock + took + behind + 1, job.last_to_core)
            pump.insert(clock + took + behind + 2, job.done, j)
            clock += took
            begun += (PACE if j > 1 else DIRECT) * took
        pump.now = 3.0
        run(pump.due())
        x_load.wait()
        a0_out = pltpu.make_async_copy(at, a0t, s_at)
        dy_load = pltpu.make_async_copy(dy_hbm, by, s_x)

        step = min(TILE, tokens)

        def norm(i, _):
            part = cols(i, step)
            normed = norm_rows(by[part, :])
            a[part, :] = normed
            at[:, part] = normed.T
            return 0

        lax.fori_loop(0, tokens // step, norm, 0)
        a0_out.start()
        pump.now = 8.0

        def gate_up(layer, gate, up, before, wgate, wup, gbuf, ubuf, actbuf, dwbuf):
            def body(step, ins, outs):
                g = nn(a[:], ins[0][:].reshape(d, TILE))
                u = nn(a[:], ins[1][:].reshape(d, TILE))
                outs[0][:] = g
                outs[1][:] = u
                product = (g * jax.nn.sigmoid(g) * u).astype(BF16)
                if layer:
                    actbuf[0] = product
                    outs[2][:] = tn(actbuf[0], by[:]).astype(BF16)
                else:
                    outs[2][:] = product

            run(pump.through(gates[layer][0]))
            later = {s: j for s, j in gates[layer].items() if s in range(1, tiles)}
            outs = piece((gate, up, act0), (gbuf, ubuf, actbuf), out_sem)
            if layer:
                outs[-1] = (lambda s: dwd1.at[cols(s, TILE), :], dwbuf, out_sem.at[2])
            stream(
                tiles,
                piece(full[layer][:PAIR], (wgate, wup), in_sem),
                outs,
                body,
                lambda: pump.plan(tiles, 3.7 if layer else 2.5, later),
                late=[s - 1 for s in later],
                before=before,
            )

        def down(wd, tall, hbuf):
            run(pump.through(gates[0]["down"]))
            wd_load = pltpu.make_async_copy(d0, wd, s_w)
            wd_load.start()

            def ready():
                a0_out.wait()
                wd_load.wait()

            def body(step, ins, outs):
                part = cols(step, rows)
                h = by[part, :] + nn(concat(ins[0], tiles), wd[:]).astype(BF16)
                outs[0][:] = h
                normed = norm_rows(h)
                a[part, :] = normed
                at[:, part] = normed.T

            stream(
                tokens // rows,
                [(lambda s: act0.at[:, cols(s, rows), :], tall, in_sem.at[0])],
                [(lambda s: h1_hbm.at[cols(s, rows), :], hbuf, out_sem.at[0])],
                body,
                lambda: pump.plan(tokens // rows, 3.8),
                before=ready,
            )
            dy_load.start()

        tile_bufs = [two(*GRID, rd, TILE)] * PAIR + [two(tokens, TILE, dtype=F32)] * PAIR + [two(tokens, TILE), two(TILE, d)]
        pl.run_scoped(functools.partial(gate_up, 0, gate0, up0, None), *tile_bufs)
        pl.run_scoped(down, pltpu.VMEM(d0.shape, BF16), two(tiles, rows, TILE), two(rows, d))
        pl.run_scoped(functools.partial(gate_up, 1, gate1, up1, dy_load.wait), *tile_bufs)
        run(pump.through(nj - 1))
        assert not pump.items
        put_down, *put_wide = scatters(place, pump, size, slots, rs_sems, acc, out, dwd1, (dwg1, dwu1), TEMPOS[0])
        put_down()
        run(pump.due())
        wg_load = pltpu.make_async_copy(g1, wg, s_w)
        wg_load.start()
        ins, grads = (gate1, up1, d1), (dwg1, dwu1)
        room = [a.at[:, pl.ds(0, TILE)]]
        pl.run_scoped(
            functools.partial(hidden, size, pump, by, at, ins, grads, (dg1, du1), room, put_wide, HID1, None, (in_sem, out_sem)), *size.hidden_bufs
        )

        def states(wu, dgbuf, dubuf, hbuf):
            wu_load = pltpu.make_async_copy(u1, wu, s_u)
            wu_load.start()

            def ready():
                wg_load.wait()
                wu_load.wait()

            def body(step, ins, outs):
                part = cols(step, few)
                dg, du, h = (ref for ref in ins)
                da = nt(concat(dg, tiles), concat(wg, tiles).reshape(d, ff)) + nt(concat(du, tiles), concat(wu, tiles).reshape(d, ff))
                by[part, :] = by[part, :] + norm_back(da.astype(BF16), h[:])

            ins = [(lambda s, ref=ref: ref.at[:, cols(s, few), :], buf, in_sem.at[k]) for k, (ref, buf) in enumerate(((dg1, dgbuf), (du1, dubuf)))]
            ins.append((lambda s: h1_hbm.at[cols(s, few), :], hbuf, in_sem.at[2]))
            stream(tokens // few, ins, [], body, lambda: pump.plan(tokens // few, STATES), before=ready)

        pl.run_scoped(states, pltpu.VMEM(wg.shape, BF16), two(tiles, few, TILE), two(tiles, few, TILE), two(few, d))
        by_out = pltpu.make_async_copy(by, dh1, s_x)
        by_out.start()

        def down_gradient(abuf, wbuf):
            def body(step, ins, outs):
                outs[0][:] = tn(ins[0][:], by[:]).astype(BF16)

            outs = [(lambda s: dwd0.at[cols(s, TILE), :], wbuf, out_sem.at[0])]
            stream(tiles, piece((act0,), (abuf,), in_sem), outs, body, lambda: pump.plan(tiles, 1.4))

        pl.run_scoped(down_gradient, two(tokens, TILE), two(TILE, d))
        pump.now = 1e9
        run(pump.due())
        for job in jobs:
            job.sent()
        by_out.wait()

    DMA = pltpu.SemaphoreType.DMA
    outs = pl.pallas_call(
        kernel,
        name="first_part",
        in_specs=[any_] * (PAIR + len(weights)),
        out_specs=[whole] * (len(weights) + 1) + [any_] * len(hbm),
        out_shape=size.blocks + [shape((8, LANES), F32)] + hbm,
        scratch_shapes=scratch
        + size.slots
        + [DMA((3, PAIR)), DMA((nj, len(Gather.SLOTS))), DMA((size.n_slots, len(Scatter.SLOTS)))]
        + [DMA((4, PAIR)), DMA((4, PAIR)), DMA((4,))],
        compiler_params=pltpu.CompilerParams(collective_id=0, has_side_effects=True, vmem_limit_bytes=66_500_000),
    )(x, dy, *weights)
    *sums, acc = outs[: len(weights) + 1]
    dh1, dwd0, gate0, up0, a0t, _, _, _, d0 = outs[len(weights) + 1 :][:9]
    return sums, acc, (dh1, dwd0, gate0, up0, a0t, d0)


def second_part(last_acc, dh1, dwd0, gate0, up0, a0t, d0):
    size = Sizes(SHARES[2], *dh1.shape, d0.shape[0])
    deep = shape(size.deep, BF16)
    n = len(size.blocks)

    def kernel(*refs):
        it = iter(refs)
        take = lambda n: [next(it) for _ in range(n)]
        acc_in, dh1_hbm, dwd0, gate0, up0, a0t, d0 = take(7)
        *out, squares = take(n + 1)
        dwg0, dwu0 = take(PAIR)
        by, at = take(PAIR)
        slots = [take(size.slot_size) for _ in range(size.n_slots)]
        acc, sums, gone, rs_sems, in_sem, out_sem, sums_sem, one_sem = take(8)
        place, pump = Place(), Pump()
        by_load, at_load = pltpu.make_async_copy(dh1_hbm, by, one_sem.at[0]), pltpu.make_async_copy(a0t, at, one_sem.at[1])
        by_load.start()
        at_load.start()
        greeting = greet(place.sharers + [place.to_diag])

        def ready():
            greeting()
            put_down()
            run(pump.due())
            acc[:] = acc_in[:]
            by_load.wait()
            at_load.wait()

        put_down, *put_wide = scatters(place, pump, size, slots, rs_sems, acc, out, dwd0, (dwg0, dwu0), TEMPOS[1])
        ins, grads = (gate0, up0, d0), (dwg0, dwu0)
        pl.run_scoped(
            functools.partial(hidden, size, pump, by, at, ins, grads, (), None, put_wide, HID0, ready, (in_sem, out_sem)), *size.hidden_bufs
        )
        pump.now = 1e9
        run(pump.due())
        sums[0] = jnp.full(acc.shape, jnp.sum(acc[:]), F32)
        hops = [[place.to_c], [place.to_x, place.to_y, place.to_diag], place.to_z]
        at_gone = 0
        for k, devices in enumerate(hops):
            for i, device in enumerate(devices):
                send(sums.at[k], gone.at[at_gone + i], sums_sem.at[len(hops)], sums_sem.at[k], device)
            await_bytes(gone.at[pl.ds(at_gone, len(devices))], sums_sem.at[k])
            total = sums[k]
            for i in range(len(devices)):
                total += gone[at_gone + i]
            at_gone += len(devices)
            if k < len(hops) - 1:
                sums[k + 1] = total
            else:
                squares[:] = total
        await_bytes(gone, sums_sem.at[len(hops)])

    DMA = pltpu.SemaphoreType.DMA
    tile = (8, LANES)
    *sums, squares = pl.pallas_call(
        kernel,
        name="second_part",
        in_specs=[whole] + [any_] * 6,
        out_specs=[whole] * (n + 1) + [any_] * PAIR,
        out_shape=size.blocks + [shape(tile, F32)] + [deep, deep],
        scratch_shapes=[pltpu.VMEM(size.thin, BF16), pltpu.VMEM(size.turned, BF16)]
        + size.slots
        + [pltpu.VMEM(tile, F32), pltpu.VMEM((3, *tile), F32), pltpu.VMEM((7, *tile), F32)]
        + [DMA((size.n_slots, len(Scatter.SLOTS))), DMA((4, PAIR)), DMA((4, PAIR)), DMA((4,)), DMA((PAIR,))],
        compiler_params=pltpu.CompilerParams(collective_id=1, has_side_effects=True, vmem_limit_bytes=66_500_000),
    )(last_acc, dh1, dwd0, gate0, up0, a0t, d0)[: n + 1]
    return sums, squares


def adamw(weights, m, v, sums, squares):
    n = len(weights)
    count = DEVICES * sum(w.size for w in weights)

    def kernel(squares_ref, *refs):
        factor = jnp.minimum(1.0, 0.5 * lax.rsqrt(squares_ref[:1, :1] / count + 1e-30))
        for k in range(n):
            w, m, v, g, last_g, new_w, new_m, new_v = refs[k::n]
            grad = jnp.where(pl.program_id(0) == 0, g[:].astype(F32), last_g[:].astype(F32)) * factor
            m_next = 0.9 * m[0] + 0.1 * grad
            v_next = 0.95 * v[0] + 0.05 * grad * grad
            wide = w[0].astype(F32)
            new_w[0] = (wide - 0.02 * (m_next * lax.rsqrt(v_next + 1e-8) + 0.1 * wide)).astype(BF16)
            new_m[0] = m_next
            new_v[0] = v_next

    blocks = [pl.BlockSpec((1, *w.shape[1:]), lambda layer: (layer, 0, 0)) for w in weights]
    once = [pl.BlockSpec(s.shape, lambda layer: (0, 0)) for s in (squares, *sums)]
    return pl.pallas_call(
        kernel,
        name="adamw",
        grid=(PAIR,),
        in_specs=once[:1] + blocks * 3 + once[1:],
        out_specs=blocks * 3,
        out_shape=[shape(w.shape, BF16) for w in weights] + [shape(w.shape, F32) for w in weights] * PAIR,
    )(squares, *weights, *m, *v, *sums)


def solution(mesh):
    def step(x, dy, *arrays):
        weights, m, v = (arrays[3 * i : 3 * i + 3] for i in range(3))
        last, acc, kept = first_part(x[0], dy[0], weights)
        sums, squares = second_part(acc, *kept)
        return tuple(adamw(weights, m, v, [*sums, *last], squares))

    states, cut = P(("rep", "dp"), None, None), P(None, "dp", None)
    return jax.shard_map(
        step,
        mesh=mesh,
        in_specs=(states, states) + (cut,) * 9,
        out_specs=(P("rep", "dp", None),) * 9,
        check_vma=False,
    )
```
